32 devices in a mesh: dp: 1 (over z), tp: 4 (over y), sp: 8 (over x, core).
Axes of the slice: x: 4, y: 4, z: 1, core: 2. Of those that a mesh axis runs over, the one named last changes fastest.
The devices are a block of a 4x4x8 slice.
Arguments:
- x_in: bfloat16 [8192, 5120], P(('dp', 'sp'), 'tp')
- w_qkv: bfloat16 [5120, 15360], P('sp', 'tp')
- w_out: bfloat16 [5120, 5120], P('sp', 'tp')
- seg_ids: int32 [8192], P(('dp', 'sp'))
Outputs:
- output: bfloat16 [8192, 5120], P(('dp', 'sp'), 'tp')
All inputs are finite; a program needn't handle non-finite values.
Results may differ from the reference program's by a relative error of at most 0.00321.
Values are sent between devices in bfloat16 or wider.
A program may use at most 768 MiB of HBM per device.

```python
import jax
import jax.numpy as jnp
from jax import lax

SEQ_LEN = 8192
HIDDEN = 5120
NUM_HEADS = 40
HEAD_DIM = 128
NUM_DOCS = 4
QUERY_BLOCK = 128


def setup_inputs(seed: int = 0, part: int = 0) -> dict:
    key_qkv, key_out = jax.random.split(jax.random.key(seed))
    part_key = jax.random.fold_in(jax.random.key(seed + 1), part)
    key_x, key_seg = jax.random.split(part_key)
    x_in = jax.random.normal(key_x, (SEQ_LEN, HIDDEN), jnp.float32)
    w_qkv = jax.random.normal(key_qkv, (HIDDEN, 3 * HIDDEN), jnp.float32) * (1.5 / HIDDEN ** 0.5)
    w_out = jax.random.normal(key_out, (HIDDEN, HIDDEN), jnp.float32) * (2.0 / HIDDEN ** 0.5)
    doc_starts = jax.random.permutation(key_seg, SEQ_LEN - 1)[: NUM_DOCS - 1] + 1
    positions = jnp.arange(SEQ_LEN, dtype=jnp.int32)
    seg_ids = jnp.sum((positions[:, None] >= doc_starts[None, :]).astype(jnp.int32), axis=1)
    return {"x_in": x_in.astype(jnp.bfloat16), "w_qkv": w_qkv.astype(jnp.bfloat16), "w_out": w_out.astype(jnp.bfloat16), "seg_ids": seg_ids.astype(jnp.int32)}


def reference(x_in, w_qkv, w_out, seg_ids):
    qkv_proj = jnp.dot(x_in, w_qkv, preferred_element_type=jnp.float32).astype(jnp.bfloat16)
    qkv_proj = qkv_proj.reshape(SEQ_LEN, NUM_HEADS, 3, HEAD_DIM).transpose(1, 2, 0, 3)
    n_blocks = SEQ_LEN // QUERY_BLOCK
    positions = jnp.arange(SEQ_LEN, dtype=jnp.int32)
    pos_query = positions.reshape(n_blocks, QUERY_BLOCK)
    seg_query = seg_ids.reshape(n_blocks, QUERY_BLOCK)
    score_scale = 1.0 / HEAD_DIM ** 0.5

    def one_head(head_qkv):
        key_head = head_qkv[1]
        value_head = head_qkv[2]
        query_blocks = head_qkv[0].reshape(n_blocks, QUERY_BLOCK, HEAD_DIM)

        def one_block(block_args):
            query_blk, pos_blk, seg_blk = block_args
            scores = jnp.dot(query_blk, key_head.T, preferred_element_type=jnp.float32) * score_scale
            allowed = (positions[None, :] <= pos_blk[:, None]) & (seg_ids[None, :] == seg_blk[:, None])
            scores = jnp.where(allowed, scores, -jnp.inf)
            prob_blk = jax.nn.softmax(scores, axis=-1).astype(jnp.bfloat16)
            return jnp.dot(prob_blk, value_head, preferred_element_type=jnp.float32).astype(jnp.bfloat16)

        return lax.map(one_block, (query_blocks, pos_query, seg_query)).reshape(SEQ_LEN, HEAD_DIM)

    context = lax.map(one_head, qkv_proj)
    context = context.transpose(1, 0, 2).reshape(SEQ_LEN, HIDDEN)
    return jnp.dot(context, w_out, preferred_element_type=jnp.float32).astype(jnp.bfloat16)
```

```python
import functools

import jax
import jax.numpy as jnp
from jax import lax
from jax.experimental import pallas as pl
from jax.experimental.pallas import tpu as pltpu
from jax.sharding import PartitionSpec as P

HEAD_DIM = 128
MESH = pl.DeviceIdType.MESH
ANY = pl.ANY
VMEM_LIMIT = 60 * 1024 * 1024


class Place:
    def __init__(self, n_tp, n_sp):
        self.n_tp, self.n_sp, self.n_x = n_tp, n_sp, n_sp // 2
        self.tp, self.sp = lax.axis_index("tp"), lax.axis_index("sp")
        self.chip, self.core = self.sp // 2, self.sp % 2
        self.sib = self.chip * 2 + 1 - self.core
        self.up, self.down = (self.tp + 1) % n_tp, (self.tp + n_tp - 1) % n_tp
        self.right, self.left = self.at(1, 0), self.at(-1, 0)

    def chip_at(self, r):
        return (self.chip + r + self.n_x) % self.n_x

    def at(self, r, d):
        return self.chip_at(r) * 2 + (self.core if d == 0 else 1 - self.core)

    def barrier(self):
        sem = pltpu.get_barrier_semaphore()
        for j in range(1, self.n_sp):
            pl.semaphore_signal(sem, inc=1, device_id={"sp": (self.sp + j) % self.n_sp}, device_id_type=MESH)
        for peer in (self.up, self.down):
            pl.semaphore_signal(sem, inc=1, device_id={"tp": peer}, device_id_type=MESH)
        pl.semaphore_wait(sem, self.n_sp + 1)


def remote(src, dst, send, recv, **peer):
    return pltpu.make_async_remote_copy(
        src_ref=src, dst_ref=dst, send_sem=send, recv_sem=recv, device_id=peer, device_id_type=MESH
    )


class Ring:
    HALF = (0, 1, 0, 1, 0, 1)

    def __init__(self, axis, me, ahead, behind, far, own, slots, rows, send, recv):
        self.half = (pl.ds(0, rows // 2), pl.ds(rows // 2, rows // 2))
        self.axis, self.me, self.ahead, self.behind, self.far = axis, me, ahead, behind, far
        self.own, self.slots, self.send, self.recv = own, slots, send, recv

    def copy(self, k):
        h = self.half[self.HALF[k]]
        if k in (2, 5):
            src = dst = self.landed(k - 2)
        else:
            src, dst = self.own.at[h], self.slots(self.me).at[h]
        peer = self.ahead if k < 3 else self.behind
        return remote(src, dst, self.send.at[k], self.recv.at[k], **{self.axis: peer})

    def landed(self, k):
        origin = (self.behind, self.behind, self.far, self.ahead, self.ahead, self.far)[k]
        return self.slots(origin).at[self.half[self.HALF[k]]]

    def start(self):
        for k in (0, 3, 1, 4):
            self.copy(k).start()

    def forward(self):
        for k in (0, 3):
            self.copy(k).wait_recv()
            self.copy(k + 2).start()

    def wait(self, *ks):
        for k in ks:
            self.copy(k).wait_recv()

    def drain(self):
        for k in range(6):
            self.copy(k).wait_send()


class WeightGather:
    def __init__(self, p, w_ref, w_all, send, recv, sib_send, sib_recv):
        self.p, self.send, self.recv = p, sib_send, sib_recv
        self.ring = Ring("sp", p.sp, p.right, p.left, p.at(2, 0), w_ref, lambda i: w_all.at[i], w_ref.shape[0],
                         send, recv)
        self.own = remote(w_ref, w_all.at[p.sp], sib_send.at[6], sib_recv.at[6], sp=p.sib)

    def start(self):
        self.ring.start()
        self.own.start()

    def to_sibling(self, k):
        block = self.ring.landed(k)
        return remote(block, block, self.send.at[k], self.recv.at[k], sp=self.p.sib)

    def forward(self):
        self.ring.forward()
        self.share(0, 3)

    def share(self, *ks):
        for k in ks:
            self.to_sibling(k).start()

    def wait_sibling(self, *ks):
        for k in ks:
            self.to_sibling(k).wait_recv()

    def drain(self):
        self.ring.drain()
        self.own.wait_send()
        for k in range(6):
            self.to_sibling(k).wait_send()


def qkv_kernel(n_tp, n_sp, x_ref, w_ref, seg_ref, m_all, skv, sq, seg_all, w_all,
               x_all, acc, qkv, w_tile, local_sem, tile_sem, ring_send, ring_recv, w_sib_send, w_sib_recv,
               seg_send, seg_recv, main_send, main_recv, kv_send, kv_recv, q_send, q_recv, own_sem):
    p = Place(n_tp, n_sp)
    rows, x_cols = x_ref.shape
    w_rows = w_ref.shape[0]
    n_tiles, _, tile = acc.shape
    head = 3 * HEAD_DIM
    n_shared = 2 * n_tiles - n_sp
    parts = n_sp // n_shared
    q_rows = rows // parts
    m_tile = min(rows, 256)
    p.barrier()

    x_own = pltpu.make_async_copy(x_ref, x_all.at[p.tp], local_sem.at[0])
    x_own.start()
    seg_own = pltpu.make_async_copy(seg_ref, seg_all.at[p.sp], local_sem.at[1])
    seg_own.start()
    x_ring = Ring("tp", p.tp, p.up, p.down, (p.tp + 2) % n_tp, x_ref, lambda i: x_all.at[i], rows,
                  ring_send.at[0], ring_recv.at[0])
    weight = WeightGather(p, w_ref, w_all, ring_send.at[1], ring_recv.at[1], w_sib_send, w_sib_recv)
    weight.start()
    x_ring.start()
    seg_copies = []
    for j in range(1, n_sp):
        copy = remote(seg_ref, seg_all.at[p.sp], seg_send.at[j - 1], seg_recv.at[j - 1], sp=(p.sp + j) % n_sp)
        copy.start()
        seg_copies.append(copy)

    def tile_load(w_src, t, slot):
        return pltpu.make_async_copy(
            w_src.at[:, pl.ds(pl.multiple_of(t * tile, tile), tile)], w_tile.at[slot], tile_sem.at[slot])

    def product(shard, m, slot):
        r = pl.ds(pl.multiple_of(m * m_tile, m_tile), m_tile)
        c = pl.ds(pl.multiple_of((shard % 2) * w_rows, w_rows), w_rows)
        return r, jnp.dot(x_all[shard // 2, r, c], w_tile[slot], preferred_element_type=jnp.float32)

    def accumulate(w_src, shard, first=False):
        tile_load(w_src, 0, 0).start()

        @pl.loop(0, n_tiles)
        def _(t):
            slot = t % 2
            tile_load(w_src, t, slot).wait()

            @pl.when(t + 1 < n_tiles)
            def _():
                tile_load(w_src, t + 1, 1 - slot).start()

            @pl.loop(0, rows // m_tile)
            def _(m):
                r, d = product(shard, m, slot)
                if first:
                    acc[t, r] = d
                else:
                    acc[t, r] += d

    x_ring.forward()
    weight.forward()
    x_ring.wait(1, 4, 2, 5)
    x_own.wait()
    accumulate(w_ref, p.sp, first=True)
    weight.own.wait_recv()
    accumulate(w_all.at[p.sib], p.sib)
    weight.ring.wait(1, 4)
    weight.share(1, 4)
    accumulate(w_all.at[p.left], p.left)
    accumulate(w_all.at[p.right], p.right)
    weight.wait_sibling(0, 1)
    accumulate(w_all.at[p.at(-1, 1)], p.at(-1, 1))
    weight.wait_sibling(3, 4)
    accumulate(w_all.at[p.at(1, 1)], p.at(1, 1))
    weight.ring.wait(2, 5)
    weight.share(2, 5)
    accumulate(w_all.at[p.at(2, 0)], p.at(2, 0))
    weight.wait_sibling(2, 5)

    last = p.at(2, 1)
    offsets = (2, 1, -1, None, 0)
    order = [n_tiles - 1 if r is None else p.chip_at(r) for r in offsets]
    pending = []
    tile_load(w_all.at[last], order[0], 0).start()
    for i, (r, t) in enumerate(zip(offsets, order)):
        slot = i % 2
        tile_load(w_all.at[last], t, slot).wait()
        if i + 1 < n_tiles:
            tile_load(w_all.at[last], order[i + 1], 1 - slot).start()

        @pl.loop(0, rows // m_tile)
        def _(m):
            rr, d = product(last, m, slot)
            qkv[t, rr] = (acc[t, rr] + d).astype(qkv.dtype)

        if r is not None:
            for d in (0, 1):
                core = p.core if d == 0 else 1 - p.core
                src = qkv.at[t, :, pl.ds(pl.multiple_of(core * head, head), head)]
                if r == 0 and d == 0:
                    copy = pltpu.make_async_copy(src, m_all.at[p.sp], own_sem.at[0])
                else:
                    j = (r % 4) * 2 + d
                    copy = remote(src, m_all.at[p.sp], main_send.at[j], main_recv.at[j], sp=p.at(r, d))
                copy.start()
                pending.append((copy, r == 0 and d == 0))
            continue
        for r2 in (2, 1, -1, 0):
            base = (p.chip_at(r2) * 2 // parts) * head
            kv_src = qkv.at[t, :, pl.ds(pl.multiple_of(base + HEAD_DIM, HEAD_DIM), 2 * HEAD_DIM)]
            if r2 == 0:
                copy = pltpu.make_async_copy(kv_src, skv.at[p.sp], own_sem.at[1])
                copy.start()
                pending.append((copy, True))
                copy = remote(kv_src, skv.at[p.sp], kv_send.at[0], kv_recv.at[0], sp=p.sib)
            else:
                copy = remote(kv_src, skv.at[p.sp], kv_send.at[r2 % 4], kv_recv.at[r2 % 4], sp=p.at(r2, 0))
            copy.start()
            if r2 == 0:
                pending.append((copy, False))
            else:
                pending.append((copy, None))
            for d in (0, 1):
                dst = p.at(r2, d)
                q_src = qkv.at[t, pl.ds(pl.multiple_of((dst % parts) * q_rows, q_rows), q_rows),
                               pl.ds(pl.multiple_of(base, HEAD_DIM), HEAD_DIM)]
                if r2 == 0 and d == 0:
                    copy = pltpu.make_async_copy(q_src, sq.at[p.sp], own_sem.at[2])
                else:
                    j = (r2 % 4) * 2 + d
                    copy = remote(q_src, sq.at[p.sp], q_send.at[j], q_recv.at[j], sp=dst)
                copy.start()
                pending.append((copy, r2 == 0 and d == 0))

    relays = []
    for r in (1, -1, 2):
        k = r % 4
        arrived = skv.at[p.at(-r, 0)]
        remote(arrived, arrived, kv_send.at[k], kv_recv.at[k], sp=p.at(r, 0)).wait_recv()
        relay = remote(arrived, arrived, kv_send.at[3 + k], kv_recv.at[3 + k], sp=p.sib)
        relay.start()
        relays.append(relay)
    for copy, local in pending:
        if local:
            copy.wait()
        else:
            copy.wait_send()
            if local is False:
                copy.wait_recv()
    for relay in relays:
        relay.wait()
    for copy in seg_copies:
        copy.wait()
    seg_own.wait()
    x_ring.drain()
    weight.drain()


def attention_kernel(scale, parts, n_main, tab, m_ref, skv_ref, sq_ref, o_ref, so_ref, vt, svt, exps, tops):
    step = pl.program_id(0)
    seq = m_ref.shape[0]
    q_tile = o_ref.shape[0]
    k_tile = 2 * q_tile
    n_bounds = tab.shape[0] - 1
    coef = scale * 1.4426950408889634
    lowest = -0.7 * float(jnp.finfo(jnp.float32).max)

    @pl.when(step == 0)
    def _():
        @pl.loop(0, seq // k_tile)
        def _(j):
            r = pl.ds(pl.multiple_of(j * k_tile, k_tile), k_tile)
            vt[j] = m_ref[r, 2 * HEAD_DIM:].T
            svt[j] = skv_ref[r, HEAD_DIM:].T

    def doc_start(row):
        start = row * 0
        for d in range(n_bounds):
            start = jnp.where(row >= tab[d], tab[d], start)
        return start

    def attend(q, k_ref, k_col, vt_ref, row0, out):
        row = row0 + lax.broadcasted_iota(jnp.int32, (1, q_tile), 1)
        start = doc_start(row)
        first = doc_start(row0) // k_tile
        diagonal = row0 // k_tile
        clear = (doc_start(row0 + q_tile - 1) + k_tile - 1) // k_tile
        clear = jnp.minimum(clear, diagonal)

        def body(masked, j, carry):
            top, total = carry
            r = pl.ds(pl.multiple_of(j * k_tile, k_tile), k_tile)
            s = lax.dot_general(k_ref[r, k_col:k_col + HEAD_DIM], q, (((1,), (1,)), ((), ())),
                                preferred_element_type=jnp.float32)
            if masked:
                key = j * k_tile + lax.broadcasted_iota(jnp.int32, s.shape, 0)
                s = jnp.where((key >= start) & (key <= row), s, lowest)
            new = jnp.maximum(top, jnp.max(s, axis=0, keepdims=True))
            e = jnp.exp2((s - new) * coef)
            exps[j] = e
            tops[j] = new
            total = total * jnp.exp2((top - new) * coef) + jnp.sum(e, axis=0, keepdims=True)
            return new, total

        def weigh(j, o):
            share = jnp.exp2((tops[j] - top) * coef) / total
            prob = (exps[j] * share).astype(jnp.bfloat16)
            return o + jnp.dot(vt_ref[j], prob, preferred_element_type=jnp.float32)

        carry = (jnp.full((1, q_tile), lowest, jnp.float32), jnp.zeros((1, q_tile), jnp.float32))
        carry = lax.fori_loop(first, clear, functools.partial(body, True), carry)
        carry = lax.fori_loop(clear, diagonal, functools.partial(body, False), carry)
        top, total = body(True, diagonal, carry)
        o = lax.fori_loop(first, diagonal + 1, weigh, jnp.zeros((HEAD_DIM, q_tile), jnp.float32))
        out[...] = o.T.astype(out.dtype)

    @pl.when(step < n_main)
    def _():
        row0 = step * q_tile
        q = m_ref[pl.ds(pl.multiple_of(row0, q_tile), q_tile), :HEAD_DIM]
        attend(q, m_ref, HEAD_DIM, vt, row0, o_ref)

    @pl.when(step >= n_main)
    def _():
        i = step - n_main
        row0 = (i * parts + tab[n_bounds]) * q_tile
        q = sq_ref[pl.ds(pl.multiple_of(i * q_tile, q_tile), q_tile), :]
        attend(q, skv_ref, 0, svt, row0, so_ref)


def out_kernel(n_tp, n_sp, o_ref, so_ref, w_ref, y_ref, ctx, w_all, acc, local_sem, w_send, w_recv, w_sib_send,
               w_sib_recv, o_send, o_recv, s_send, s_recv, c_send, c_recv):
    p = Place(n_tp, n_sp)
    n_x = p.n_x
    _, rows, local = ctx.shape
    w_rows = w_ref.shape[0]
    n_shared = local // HEAD_DIM - n_sp
    parts = n_sp // n_shared
    q_rows = rows // parts
    m_tile = min(rows, 256)
    pair = 2 * HEAD_DIM
    p.barrier()

    w_own = pltpu.make_async_copy(w_ref, w_all.at[p.sp], local_sem.at[0])
    w_own.start()

    def head_copy(r, d):
        dst = p.at(r, d)
        src = o_ref.at[pl.ds(pl.multiple_of(dst * rows, rows), rows)]
        to = ctx.at[p.tp, :, pl.ds(pl.multiple_of(p.sp * HEAD_DIM, HEAD_DIM), HEAD_DIM)]
        if r == 0 and d == 0:
            return pltpu.make_async_copy(src, to, local_sem.at[1])
        j = (r % 4) * 2 + d
        return remote(src, to, o_send.at[j], o_recv.at[j], sp=dst)

    def shared_copy(r, d):
        dst = p.at(r, d)
        src = so_ref.at[pl.ds(pl.multiple_of(dst * q_rows, q_rows), q_rows)]
        to = ctx.at[p.tp, pl.ds(pl.multiple_of((p.sp % parts) * q_rows, q_rows), q_rows),
                    pl.ds(pl.multiple_of((n_sp + p.sp // parts) * HEAD_DIM, HEAD_DIM), HEAD_DIM)]
        if r == 0 and d == 0:
            return pltpu.make_async_copy(src, to, local_sem.at[2])
        j = (r % 4) * 2 + d
        return remote(src, to, s_send.at[j], s_recv.at[j], sp=dst)

    peers = [(r, d) for r in (0, 1, -1, 2) for d in (0, 1)]
    for r, d in peers:
        head_copy(r, d).start()
    for r, d in peers:
        shared_copy(r, d).start()
    weight = WeightGather(p, w_ref, w_all, w_send, w_recv, w_sib_send, w_sib_recv)
    weight.start()

    def ring(i, column):
        c = pl.ds(pl.multiple_of(column, pair), pair)
        return Ring("tp", p.tp, p.up, p.down, (p.tp + 2) % n_tp, ctx.at[p.tp, :, c], lambda j: ctx.at[j, :, c], rows,
                    c_send.at[i], c_recv.at[i])

    def wait_in(copy, local):
        if local:
            copy.wait()
        else:
            copy.wait_recv()

    rings = []
    for i, r in enumerate((0, 1, -1, 2)):
        for d in (0, 1):
            wait_in(head_copy(r, d), r == 0 and d == 0)
        rings.append(ring(i, p.chip_at(-r) * pair))
        rings[-1].start()
    for r, d in peers:
        wait_in(shared_copy(r, d), r == 0 and d == 0)
    rings.append(ring(n_x, n_sp * HEAD_DIM))
    rings[-1].start()
    for c in rings:
        c.forward()
    weight.forward()
    weight.ring.wait(1, 4)
    weight.share(1, 4)
    for c in rings:
        c.wait(1, 4)
    w_own.wait()
    weight.own.wait_recv()
    weight.wait_sibling(0, 1, 3, 4)

    def block(j, step):
        @pl.loop(0, rows // m_tile)
        def _(m):
            r = pl.ds(pl.multiple_of(m * m_tile, m_tile), m_tile)
            d = jnp.dot(ctx[j, r, :w_rows], w_all[2 * j], preferred_element_type=jnp.float32)
            d += jnp.dot(ctx[j, r, w_rows:], w_all[2 * j + 1], preferred_element_type=jnp.float32)
            if step == 0:
                acc[r] = d
            elif step < n_tp - 1:
                acc[r] += d
            else:
                y_ref[r] = (acc[r] + d).astype(y_ref.dtype)

    turn = (p.chip + n_x - p.tp) % n_x
    far = turn // 2
    block((p.tp + far * (1 - turn % 2)) % n_tp, 0)
    block((p.tp + 1 + 2 * far) % n_tp, 1)
    weight.ring.wait(2, 5)
    weight.share(2, 5)
    weight.wait_sibling(2, 5)
    block((p.tp + far * (turn - 2) + (1 - far) * 3) % n_tp, 2)
    for c in rings:
        c.wait(2, 5)
    block((p.tp + 2) % n_tp, 3)

    for c in rings:
        c.drain()
    weight.drain()
    for r, d in peers:
        if not (r == 0 and d == 0):
            head_copy(r, d).wait_send()
            shared_copy(r, d).wait_send()


def solution(mesh):
    n_tp, n_sp = mesh.shape["tp"], mesh.shape["sp"]
    dma = pltpu.SemaphoreType.DMA
    hbm = pl.BlockSpec(memory_space=ANY)

    def params(collective_id):
        return pltpu.CompilerParams(collective_id=collective_id, has_side_effects=True, vmem_limit_bytes=VMEM_LIMIT)

    def local_block(x_blk, wqkv_blk, wout_blk, seg_blk):
        rows, x_cols = x_blk.shape
        w_rows, n_cols = wqkv_blk.shape
        head = 3 * HEAD_DIM
        heads = n_cols // head
        local = heads * HEAD_DIM
        n_shared = heads - n_sp
        parts = n_sp // n_shared
        q_rows = rows // parts
        tile = 2 * head
        n_tiles = n_cols // tile
        seq = n_sp * rows
        bf16 = x_blk.dtype
        n_docs = 4

        seg = seg_blk.reshape(rows // 128, 128)
        m_all, skv, sq, seg_all, _ = pl.pallas_call(
            functools.partial(qkv_kernel, n_tp, n_sp),
            out_shape=(
                jax.ShapeDtypeStruct((n_sp, rows, head), bf16),
                jax.ShapeDtypeStruct((n_sp, rows, 2 * HEAD_DIM), bf16),
                jax.ShapeDtypeStruct((n_sp, q_rows, HEAD_DIM), bf16),
                jax.ShapeDtypeStruct((n_sp,) + seg.shape, seg.dtype),
                jax.ShapeDtypeStruct((n_sp, w_rows, n_cols), bf16),
            ),
            in_specs=[hbm] * 3,
            out_specs=(hbm,) * 5,
            scratch_shapes=[
                pltpu.VMEM((n_tp, rows, x_cols), bf16),
                pltpu.VMEM((n_tiles, rows, tile), jnp.float32),
                pltpu.VMEM((n_tiles, rows, tile), bf16),
                pltpu.VMEM((2, w_rows, tile), bf16),
                dma((2,)), dma((2,)), dma((2, 6)), dma((2, 6)), dma((7,)), dma((7,)),
                dma((n_sp - 1,)), dma((n_sp - 1,)), dma((8,)), dma((8,)), dma((7,)), dma((7,)), dma((8,)), dma((8,)),
                dma((3,)),
            ],
            compiler_params=params(0),
            name="qkv",
        )(x_blk, wqkv_blk, seg)

        starts = jnp.sum((seg_all.reshape(1, seq) < jnp.arange(1, n_docs, dtype=seg_all.dtype)[:, None]).astype(jnp.int32),
                         axis=1)
        table = jnp.concatenate([starts, (lax.axis_index("sp") % parts).astype(jnp.int32)[None]])
        n_main = seq // q_rows

        def whole(shape):
            return pl.BlockSpec(shape, lambda i, t: (0, 0), pipeline_mode=pl.Buffered(1))

        o_main, o_shared = pl.pallas_call(
            functools.partial(attention_kernel, 1.0 / HEAD_DIM ** 0.5, parts, n_main),
            out_shape=(jax.ShapeDtypeStruct((seq, HEAD_DIM), bf16), jax.ShapeDtypeStruct((seq // parts, HEAD_DIM), bf16)),
            grid_spec=pltpu.PrefetchScalarGridSpec(
                num_scalar_prefetch=1,
                grid=(n_main + n_main // parts,),
                in_specs=[whole((seq, head)), whole((seq, 2 * HEAD_DIM)), whole((seq // parts, HEAD_DIM))],
                out_specs=(pl.BlockSpec((q_rows, HEAD_DIM), lambda i, t: (jnp.minimum(i, n_main - 1), 0)),
                           pl.BlockSpec((q_rows, HEAD_DIM), lambda i, t: (jnp.maximum(i - n_main, 0), 0))),
                scratch_shapes=[pltpu.VMEM((seq // (2 * q_rows), HEAD_DIM, 2 * q_rows), bf16)] * 2 + [
                    pltpu.VMEM((seq // (2 * q_rows), 2 * q_rows, q_rows), jnp.float32),
                    pltpu.VMEM((seq // (2 * q_rows), 1, q_rows), jnp.float32),
                ],
            ),
            compiler_params=pltpu.CompilerParams(dimension_semantics=("arbitrary",), vmem_limit_bytes=VMEM_LIMIT),
            name="attention",
        )(table, m_all.reshape(seq, head), skv.reshape(seq, 2 * HEAD_DIM), sq.reshape(seq // parts, HEAD_DIM))

        wo_rows, wo_cols = wout_blk.shape
        n_rings = local // (2 * HEAD_DIM)
        return pl.pallas_call(
            functools.partial(out_kernel, n_tp, n_sp),
            out_shape=jax.ShapeDtypeStruct((rows, wo_cols), bf16),
            in_specs=[hbm] * 3,
            out_specs=pl.BlockSpec(memory_space=pltpu.VMEM),
            scratch_shapes=[
                pltpu.VMEM((n_tp, rows, local), bf16),
                pltpu.VMEM((n_sp, wo_rows, wo_cols), bf16),
                pltpu.VMEM((rows, wo_cols), jnp.float32),
                dma((3,)), dma((6,)), dma((6,)), dma((7,)), dma((7,)),
                dma((8,)), dma((8,)), dma((8,)), dma((8,)), dma((n_rings, 6)), dma((n_rings, 6)),
            ],
            compiler_params=params(1),
            name="out",
        )(o_main, o_shared, wout_blk)

    row_spec = P(("dp", "sp"), "tp")
    return jax.shard_map(
        local_block, mesh=mesh, in_specs=(row_spec, P("sp", "tp"), P("sp", "tp"), P(("dp", "sp"))),
        out_specs=row_spec, check_vma=False)
```

```python
import functools

import jax
import jax.numpy as jnp
from jax import lax
from jax.experimental import pallas as pl
from jax.experimental.pallas import tpu as pltpu
from jax.sharding import PartitionSpec as P

HEAD_DIM = 128
MESH = pl.DeviceIdType.MESH
ANY = pl.ANY
VMEM_LIMIT = 60 * 1024 * 1024


class Place:
    def __init__(self, n_tp, n_sp):
        self.n_tp, self.n_sp, self.n_x = n_tp, n_sp, n_sp // 2
        self.tp, self.sp = lax.axis_index("tp"), lax.axis_index("sp")
        self.chip, self.core = self.sp // 2, self.sp % 2
        self.sib = self.chip * 2 + 1 - self.core
        self.up, self.down = (self.tp + 1) % n_tp, (self.tp + n_tp - 1) % n_tp
        self.right, self.left = self.at(1, 0), self.at(-1, 0)

    def chip_at(self, r):
        return (self.chip + r + self.n_x) % self.n_x

    def at(self, r, d):
        return self.chip_at(r) * 2 + (self.core if d == 0 else 1 - self.core)

    def barrier(self):
        sem = pltpu.get_barrier_semaphore()
        for j in range(1, self.n_sp):
            pl.semaphore_signal(sem, inc=1, device_id={"sp": (self.sp + j) % self.n_sp}, device_id_type=MESH)
        for peer in (self.up, self.down):
            pl.semaphore_signal(sem, inc=1, device_id={"tp": peer}, device_id_type=MESH)
        pl.semaphore_wait(sem, self.n_sp + 1)


def remote(src, dst, send, recv, **peer):
    return pltpu.make_async_remote_copy(
        src_ref=src, dst_ref=dst, send_sem=send, recv_sem=recv, device_id=peer, device_id_type=MESH
    )


class Ring:
    HALF = (0, 1, 0, 1, 0, 1)

    def __init__(self, axis, me, ahead, behind, far, own, slots, rows, send, recv):
        self.half = (pl.ds(0, rows // 2), pl.ds(rows // 2, rows // 2))
        self.axis, self.me, self.ahead, self.behind, self.far = axis, me, ahead, behind, far
        self.own, self.slots, self.send, self.recv = own, slots, send, recv

    def copy(self, k):
        h = self.half[self.HALF[k]]
        if k in (2, 5):
            src = dst = self.landed(k - 2)
        else:
            src, dst = self.own.at[h], self.slots(self.me).at[h]
        peer = self.ahead if k < 3 else self.behind
        return remote(src, dst, self.send.at[k], self.recv.at[k], **{self.axis: peer})

    def landed(self, k):
        origin = (self.behind, self.behind, self.far, self.ahead, self.ahead, self.far)[k]
        return self.slots(origin).at[self.half[self.HALF[k]]]

    def start(self):
        for k in (0, 3, 1, 4):
            self.copy(k).start()

    def forward(self):
        for k in (0, 3):
            self.copy(k).wait_recv()
            self.copy(k + 2).start()

    def wait(self, *ks):
        for k in ks:
            self.copy(k).wait_recv()

    def drain(self):
        for k in range(6):
            self.copy(k).wait_send()


class WeightGather:
    def __init__(self, p, w_ref, w_all, send, recv, sib_send, sib_recv):
        self.p, self.send, self.recv = p, sib_send, sib_recv
        self.ring = Ring("sp", p.sp, p.right, p.left, p.at(2, 0), w_ref, lambda i: w_all.at[i], w_ref.shape[0],
                         send, recv)
        self.own = remote(w_ref, w_all.at[p.sp], sib_send.at[6], sib_recv.at[6], sp=p.sib)

    def start(self):
        self.ring.start()
        self.own.start()

    def to_sibling(self, k):
        block = self.ring.landed(k)
        return remote(block, block, self.send.at[k], self.recv.at[k], sp=self.p.sib)

    def forward(self):
        self.ring.forward()
        self.share(0, 3)

    def share(self, *ks):
        for k in ks:
            self.to_sibling(k).start()

    def wait_sibling(self, *ks):
        for k in ks:
            self.to_sibling(k).wait_recv()

    def drain(self):
        self.ring.drain()
        self.own.wait_send()
        for k in range(6):
            self.to_sibling(k).wait_send()


def qkv_kernel(n_tp, n_sp, x_ref, w_ref, seg_ref, m_all, skv, sq, seg_all, w_all,
               x_all, acc, qkv, w_tile, local_sem, tile_sem, ring_send, ring_recv, w_sib_send, w_sib_recv,
               seg_send, seg_recv, main_send, main_recv, kv_send, kv_recv, q_send, q_recv, own_sem):
    p = Place(n_tp, n_sp)
    rows, x_cols = x_ref.shape
    w_rows = w_ref.shape[0]
    n_tiles, _, tile = acc.shape
    head = 3 * HEAD_DIM
    n_shared = 2 * n_tiles - n_sp
    parts = n_sp // n_shared
    q_rows = rows // parts
    m_tile = min(rows, 256)
    p.barrier()

    x_own = pltpu.make_async_copy(x_ref, x_all.at[p.tp], local_sem.at[0])
    x_own.start()
    seg_own = pltpu.make_async_copy(seg_ref, seg_all.at[p.sp], local_sem.at[1])
    seg_own.start()
    x_ring = Ring("tp", p.tp, p.up, p.down, (p.tp + 2) % n_tp, x_ref, lambda i: x_all.at[i], rows,
                  ring_send.at[0], ring_recv.at[0])
    weight = WeightGather(p, w_ref, w_all, ring_send.at[1], ring_recv.at[1], w_sib_send, w_sib_recv)
    weight.start()
    x_ring.start()
    seg_copies = []
    for j in range(1, n_sp):
        copy = remote(seg_ref, seg_all.at[p.sp], seg_send.at[j - 1], seg_recv.at[j - 1], sp=(p.sp + j) % n_sp)
        copy.start()
        seg_copies.append(copy)

    def tile_load(w_src, t, slot):
        return pltpu.make_async_copy(
            w_src.at[:, pl.ds(pl.multiple_of(t * tile, tile), tile)], w_tile.at[slot], tile_sem.at[slot])

    def product(shard, m, slot):
        r = pl.ds(pl.multiple_of(m * m_tile, m_tile), m_tile)
        c = pl.ds(pl.multiple_of((shard % 2) * w_rows, w_rows), w_rows)
        return r, jnp.dot(x_all[shard // 2, r, c], w_tile[slot], preferred_element_type=jnp.float32)

    def accumulate(w_src, shard, first=False):
        tile_load(w_src, 0, 0).start()

        @pl.loop(0, n_tiles)
        def _(t):
            slot = t % 2
            tile_load(w_src, t, slot).wait()

            @pl.when(t + 1 < n_tiles)
            def _():
                tile_load(w_src, t + 1, 1 - slot).start()

            @pl.loop(0, rows // m_tile)
            def _(m):
                r, d = product(shard, m, slot)
                if first:
                    acc[t, r] = d
                else:
                    acc[t, r] += d

    x_ring.forward()
    weight.forward()
    x_ring.wait(1, 4, 2, 5)
    x_own.wait()
    accumulate(w_ref, p.sp, first=True)
    weight.own.wait_recv()
    accumulate(w_all.at[p.sib], p.sib)
    weight.ring.wait(1, 4)
    weight.share(1, 4)
    accumulate(w_all.at[p.left], p.left)
    accumulate(w_all.at[p.right], p.right)
    weight.wait_sibling(0, 1)
    accumulate(w_all.at[p.at(-1, 1)], p.at(-1, 1))
    weight.wait_sibling(3, 4)
    accumulate(w_all.at[p.at(1, 1)], p.at(1, 1))
    weight.ring.wait(2, 5)
    weight.share(2, 5)
    accumulate(w_all.at[p.at(2, 0)], p.at(2, 0))
    weight.wait_sibling(2, 5)

    last = p.at(2, 1)
    offsets = (2, 1, -1, None, 0)
    order = [n_tiles - 1 if r is None else p.chip_at(r) for r in offsets]
    pending = []
    tile_load(w_all.at[last], order[0], 0).start()
    for i, (r, t) in enumerate(zip(offsets, order)):
        slot = i % 2
        tile_load(w_all.at[last], t, slot).wait()
        if i + 1 < n_tiles:
            tile_load(w_all.at[last], order[i + 1], 1 - slot).start()

        @pl.loop(0, rows // m_tile)
        def _(m):
            rr, d = product(last, m, slot)
            qkv[t, rr] = (acc[t, rr] + d).astype(qkv.dtype)

        if r is not None:
            for d in (0, 1):
                core = p.core if d == 0 else 1 - p.core
                src = qkv.at[t, :, pl.ds(pl.multiple_of(core * head, head), head)]
                if r == 0 and d == 0:
                    copy = pltpu.make_async_copy(src, m_all.at[p.sp], own_sem.at[0])
                else:
                    j = (r % 4) * 2 + d
                    copy = remote(src, m_all.at[p.sp], main_send.at[j], main_recv.at[j], sp=p.at(r, d))
                copy.start()
                pending.append((copy, r == 0 and d == 0))
            continue
        for r2 in (2, 1, -1, 0):
            base = (p.chip_at(r2) * 2 // parts) * head
            kv_src = qkv.at[t, :, pl.ds(pl.multiple_of(base + HEAD_DIM, HEAD_DIM), 2 * HEAD_DIM)]
            if r2 == 0:
                copy = pltpu.make_async_copy(kv_src, skv.at[p.sp], own_sem.at[1])
                copy.start()
                pending.append((copy, True))
                copy = remote(kv_src, skv.at[p.sp], kv_send.at[0], kv_recv.at[0], sp=p.sib)
            else:
                copy = remote(kv_src, skv.at[p.sp], kv_send.at[r2 % 4], kv_recv.at[r2 % 4], sp=p.at(r2, 0))
            copy.start()
            if r2 == 0:
                pending.append((copy, False))
            else:
                pending.append((copy, None))
            for d in (0, 1):
                dst = p.at(r2, d)
                q_src = qkv.at[t, pl.ds(pl.multiple_of((dst % parts) * q_rows, q_rows), q_rows),
                               pl.ds(pl.multiple_of(base, HEAD_DIM), HEAD_DIM)]
                if r2 == 0 and d == 0:
                    copy = pltpu.make_async_copy(q_src, sq.at[p.sp], own_sem.at[2])
                else:
                    j = (r2 % 4) * 2 + d
                    copy = remote(q_src, sq.at[p.sp], q_send.at[j], q_recv.at[j], sp=dst)
                copy.start()
                pending.append((copy, r2 == 0 and d == 0))

    relays = []
    for r in (1, -1, 2):
        k = r % 4
        arrived = skv.at[p.at(-r, 0)]
        remote(arrived, arrived, kv_send.at[k], kv_recv.at[k], sp=p.at(r, 0)).wait_recv()
        relay = remote(arrived, arrived, kv_send.at[3 + k], kv_recv.at[3 + k], sp=p.sib)
        relay.start()
        relays.append(relay)
    for copy, local in pending:
        if local:
            copy.wait()
        else:
            copy.wait_send()
            if local is False:
                copy.wait_recv()
    for relay in relays:
        relay.wait()
    for copy in seg_copies:
        copy.wait()
    seg_own.wait()
    x_ring.drain()
    weight.drain()


def attention_kernel(scale, parts, n_main, tab, m_ref, skv_ref, sq_ref, o_ref, so_ref, vt, svt, scores, exps, probs,
                     tops):
    step = pl.program_id(0)
    seq = m_ref.shape[0]
    _, k_tile, _ = exps.shape
    n_bounds = tab.shape[0] - 1
    coef = scale * 1.4426950408889634
    lowest = -0.7 * float(jnp.finfo(jnp.float32).max)

    @pl.when(step == 0)
    def _():
        @pl.loop(0, seq // k_tile)
        def _(j):
            r = pl.ds(pl.multiple_of(j * k_tile, k_tile), k_tile)
            vt[j] = m_ref[r, 2 * HEAD_DIM:].T
            svt[j] = skv_ref[r, HEAD_DIM:].T

    def doc_start(row):
        start = row * 0
        for d in range(n_bounds):
            start = jnp.where(row >= tab[d], tab[d], start)
        return start

    def attend(q, k_ref, k_col, vt_ref, row0, out):
        q_tile = q.shape[0]
        lanes = slice(0, q_tile)
        row = row0 + lax.broadcasted_iota(jnp.int32, (1, q_tile), 1)
        start = doc_start(row)
        first = doc_start(row0) // k_tile
        last = row0 // k_tile
        clear = (doc_start(row0 + q_tile - 1) + k_tile - 1) // k_tile
        clear = jnp.minimum(clear, last)

        def score(j):
            r = pl.ds(pl.multiple_of(j * k_tile, k_tile), k_tile)
            scores[:, lanes] = lax.dot_general(k_ref[r, k_col:k_col + HEAD_DIM], q, (((1,), (1,)), ((), ())),
                                               preferred_element_type=jnp.float32)

        def body(edge, j, carry):
            top, total = carry
            s = scores[:, lanes]
            if edge != "last":
                score(j + 1)
            if edge:
                key = j * k_tile + lax.broadcasted_iota(jnp.int32, s.shape, 0)
                seen = key >= start
                if edge == "last":
                    seen &= key <= row
                s = jnp.where(seen, s, lowest)
            new = jnp.maximum(top, jnp.max(s, axis=0, keepdims=True))
            e = jnp.exp2((s - new) * coef)
            exps[j, :, lanes] = e
            tops[j, :, lanes] = new
            total = total * jnp.exp2((top - new) * coef) + jnp.sum(e, axis=0, keepdims=True)
            return new, total

        carry = (jnp.full((1, q_tile), lowest, jnp.float32), jnp.zeros((1, q_tile), jnp.float32))
        score(first)
        carry = lax.fori_loop(first, clear, functools.partial(body, "first"), carry)
        carry = lax.fori_loop(clear, last, functools.partial(body, ""), carry)
        top, total = body("last", last, carry)
        inverse = 1.0 / total

        def prob(j):
            share = jnp.exp2((tops[j, :, lanes] - top) * coef) * inverse
            return (exps[j, :, lanes] * share).astype(jnp.bfloat16)

        def weigh(j, o):
            p = probs[:, lanes]
            probs[:, lanes] = prob(j + 1)
            return o + jnp.dot(vt_ref[j], p, preferred_element_type=jnp.float32)

        probs[:, lanes] = prob(first)
        o = lax.fori_loop(first, last, weigh, jnp.zeros((HEAD_DIM, q_tile), jnp.float32))
        o = o + jnp.dot(vt_ref[last], probs[:, lanes], preferred_element_type=jnp.float32)
        out[...] = o.T.astype(out.dtype)

    @pl.when(step < n_main)
    def _():
        q_tile = o_ref.shape[0]
        row0 = step * q_tile
        q = m_ref[pl.ds(pl.multiple_of(row0, q_tile), q_tile), :HEAD_DIM]
        attend(q, m_ref, HEAD_DIM, vt, row0, o_ref)

    @pl.when(step >= n_main)
    def _():
        q_tile = so_ref.shape[0]
        i = step - n_main
        row0 = (i * parts + tab[n_bounds]) * q_tile
        q = sq_ref[pl.ds(pl.multiple_of(i * q_tile, q_tile), q_tile), :]
        attend(q, skv_ref, 0, svt, row0, so_ref)


def out_kernel(n_tp, n_sp, o_ref, so_ref, w_ref, y_ref, ctx, w_all, acc, local_sem, w_send, w_recv, w_sib_send,
               w_sib_recv, o_send, o_recv, s_send, s_recv, c_send, c_recv):
    p = Place(n_tp, n_sp)
    n_x = p.n_x
    _, rows, local = ctx.shape
    w_rows = w_ref.shape[0]
    n_shared = local // HEAD_DIM - n_sp
    parts = n_sp // n_shared
    q_rows = rows // parts
    m_tile = min(rows, 256)
    pair = 2 * HEAD_DIM
    p.barrier()

    w_own = pltpu.make_async_copy(w_ref, w_all.at[p.sp], local_sem.at[0])
    w_own.start()

    def head_copy(r, d):
        dst = p.at(r, d)
        src = o_ref.at[pl.ds(pl.multiple_of(dst * rows, rows), rows)]
        to = ctx.at[p.tp, :, pl.ds(pl.multiple_of(p.sp * HEAD_DIM, HEAD_DIM), HEAD_DIM)]
        if r == 0 and d == 0:
            return pltpu.make_async_copy(src, to, local_sem.at[1])
        j = (r % 4) * 2 + d
        return remote(src, to, o_send.at[j], o_recv.at[j], sp=dst)

    def shared_copy(r, d):
        dst = p.at(r, d)
        src = so_ref.at[pl.ds(pl.multiple_of(dst * q_rows, q_rows), q_rows)]
        to = ctx.at[p.tp, pl.ds(pl.multiple_of((p.sp % parts) * q_rows, q_rows), q_rows),
                    pl.ds(pl.multiple_of((n_sp + p.sp // parts) * HEAD_DIM, HEAD_DIM), HEAD_DIM)]
        if r == 0 and d == 0:
            return pltpu.make_async_copy(src, to, local_sem.at[2])
        j = (r % 4) * 2 + d
        return remote(src, to, s_send.at[j], s_recv.at[j], sp=dst)

    peers = [(r, d) for r in (0, 1, -1, 2) for d in (0, 1)]
    for r, d in peers:
        head_copy(r, d).start()
    for r, d in peers:
        shared_copy(r, d).start()
    weight = WeightGather(p, w_ref, w_all, w_send, w_recv, w_sib_send, w_sib_recv)
    weight.start()

    def ring(i, column):
        c = pl.ds(pl.multiple_of(column, pair), pair)
        return Ring("tp", p.tp, p.up, p.down, (p.tp + 2) % n_tp, ctx.at[p.tp, :, c], lambda j: ctx.at[j, :, c], rows,
                    c_send.at[i], c_recv.at[i])

    def wait_in(copy, local):
        if local:
            copy.wait()
        else:
            copy.wait_recv()

    rings = []
    for i, r in enumerate((0, 1, -1, 2)):
        for d in (0, 1):
            wait_in(head_copy(r, d), r == 0 and d == 0)
        rings.append(ring(i, p.chip_at(-r) * pair))
        rings[-1].start()
    for r, d in peers:
        wait_in(shared_copy(r, d), r == 0 and d == 0)
    rings.append(ring(n_x, n_sp * HEAD_DIM))
    rings[-1].start()
    for c in rings:
        c.forward()
    weight.forward()
    weight.ring.wait(1, 4)
    weight.share(1, 4)
    for c in rings:
        c.wait(1, 4)
    w_own.wait()
    weight.own.wait_recv()
    weight.wait_sibling(0, 1, 3, 4)

    def block(j, step):
        @pl.loop(0, rows // m_tile)
        def _(m):
            r = pl.ds(pl.multiple_of(m * m_tile, m_tile), m_tile)
            d = jnp.dot(ctx[j, r, :w_rows], w_all[2 * j], preferred_element_type=jnp.float32)
            d += jnp.dot(ctx[j, r, w_rows:], w_all[2 * j + 1], preferred_element_type=jnp.float32)
            if step == 0:
                acc[r] = d
            elif step < n_tp - 1:
                acc[r] += d
            else:
                y_ref[r] = (acc[r] + d).astype(y_ref.dtype)

    turn = (p.chip + n_x - p.tp) % n_x
    far = turn // 2
    block((p.tp + far * (1 - turn % 2)) % n_tp, 0)
    block((p.tp + 1 + 2 * far) % n_tp, 1)
    weight.ring.wait(2, 5)
    weight.share(2, 5)
    weight.wait_sibling(2, 5)
    block((p.tp + far * (turn - 2) + (1 - far) * 3) % n_tp, 2)
    for c in rings:
        c.wait(2, 5)
    block((p.tp + 2) % n_tp, 3)

    for c in rings:
        c.drain()
    weight.drain()
    for r, d in peers:
        if not (r == 0 and d == 0):
            head_copy(r, d).wait_send()
            shared_copy(r, d).wait_send()


def solution(mesh):
    n_tp, n_sp = mesh.shape["tp"], mesh.shape["sp"]
    dma = pltpu.SemaphoreType.DMA
    hbm = pl.BlockSpec(memory_space=ANY)

    def params(collective_id):
        return pltpu.CompilerParams(collective_id=collective_id, has_side_effects=True, vmem_limit_bytes=VMEM_LIMIT)

    def local_block(x_blk, wqkv_blk, wout_blk, seg_blk):
        rows, x_cols = x_blk.shape
        w_rows, n_cols = wqkv_blk.shape
        head = 3 * HEAD_DIM
        heads = n_cols // head
        local = heads * HEAD_DIM
        n_shared = heads - n_sp
        parts = n_sp // n_shared
        q_rows = rows // parts
        tile = 2 * head
        n_tiles = n_cols // tile
        seq = n_sp * rows
        bf16 = x_blk.dtype
        n_docs = 4

        seg = seg_blk.reshape(rows // 128, 128)
        m_all, skv, sq, seg_all, _ = pl.pallas_call(
            functools.partial(qkv_kernel, n_tp, n_sp),
            out_shape=(
                jax.ShapeDtypeStruct((n_sp, rows, head), bf16),
                jax.ShapeDtypeStruct((n_sp, rows, 2 * HEAD_DIM), bf16),
                jax.ShapeDtypeStruct((n_sp, q_rows, HEAD_DIM), bf16),
                jax.ShapeDtypeStruct((n_sp,) + seg.shape, seg.dtype),
                jax.ShapeDtypeStruct((n_sp, w_rows, n_cols), bf16),
            ),
            in_specs=[hbm] * 3,
            out_specs=(hbm,) * 5,
            scratch_shapes=[
                pltpu.VMEM((n_tp, rows, x_cols), bf16),
                pltpu.VMEM((n_tiles, rows, tile), jnp.float32),
                pltpu.VMEM((n_tiles, rows, tile), bf16),
                pltpu.VMEM((2, w_rows, tile), bf16),
                dma((2,)), dma((2,)), dma((2, 6)), dma((2, 6)), dma((7,)), dma((7,)),
                dma((n_sp - 1,)), dma((n_sp - 1,)), dma((8,)), dma((8,)), dma((7,)), dma((7,)), dma((8,)), dma((8,)),
                dma((3,)),
            ],
            compiler_params=params(0),
            name="qkv",
        )(x_blk, wqkv_blk, seg)

        starts = jnp.sum((seg_all.reshape(1, seq) < jnp.arange(1, n_docs, dtype=seg_all.dtype)[:, None]).astype(jnp.int32),
                         axis=1)
        table = jnp.concatenate([starts, (lax.axis_index("sp") % parts).astype(jnp.int32)[None]])
        q_tile = k_tile = 2 * q_rows
        n_main, n_side, n_keys = seq // q_tile, n_sp, seq // k_tile

        def whole(shape):
            return pl.BlockSpec(shape, lambda i, t: (0, 0), pipeline_mode=pl.Buffered(1))

        o_main, o_shared = pl.pallas_call(
            functools.partial(attention_kernel, 1.0 / HEAD_DIM ** 0.5, parts, n_main),
            out_shape=(jax.ShapeDtypeStruct((seq, HEAD_DIM), bf16), jax.ShapeDtypeStruct((seq // parts, HEAD_DIM), bf16)),
            grid_spec=pltpu.PrefetchScalarGridSpec(
                num_scalar_prefetch=1,
                grid=(n_main + n_side,),
                in_specs=[whole((seq, head)), whole((seq, 2 * HEAD_DIM)), whole((seq // parts, HEAD_DIM))],
                out_specs=(pl.BlockSpec((q_tile, HEAD_DIM), lambda i, t: (jnp.minimum(i, n_main - 1), 0)),
                           pl.BlockSpec((q_rows, HEAD_DIM), lambda i, t: (jnp.maximum(i - n_main, 0), 0))),
                scratch_shapes=[
                    pltpu.VMEM((n_keys, HEAD_DIM, k_tile), bf16),
                    pltpu.VMEM((n_keys, HEAD_DIM, k_tile), bf16),
                    pltpu.VMEM((k_tile, q_tile), jnp.float32),
                    pltpu.VMEM((n_keys, k_tile, q_tile), jnp.float32),
                    pltpu.VMEM((k_tile, q_tile), bf16),
                    pltpu.VMEM((n_keys, 1, q_tile), jnp.float32),
                ],
            ),
            compiler_params=pltpu.CompilerParams(dimension_semantics=("arbitrary",), vmem_limit_bytes=VMEM_LIMIT),
            name="attention",
        )(table, m_all.reshape(seq, head), skv.reshape(seq, 2 * HEAD_DIM), sq.reshape(seq // parts, HEAD_DIM))

        wo_rows, wo_cols = wout_blk.shape
        n_rings = local // (2 * HEAD_DIM)
        return pl.pallas_call(
            functools.partial(out_kernel, n_tp, n_sp),
            out_shape=jax.ShapeDtypeStruct((rows, wo_cols), bf16),
            in_specs=[hbm] * 3,
            out_specs=pl.BlockSpec(memory_space=pltpu.VMEM),
            scratch_shapes=[
                pltpu.VMEM((n_tp, rows, local), bf16),
                pltpu.VMEM((n_sp, wo_rows, wo_cols), bf16),
                pltpu.VMEM((rows, wo_cols), jnp.float32),
                dma((3,)), dma((6,)), dma((6,)), dma((7,)), dma((7,)),
                dma((8,)), dma((8,)), dma((8,)), dma((8,)), dma((n_rings, 6)), dma((n_rings, 6)),
            ],
            compiler_params=params(1),
            name="out",
        )(o_main, o_shared, wout_blk)

    row_spec = P(("dp", "sp"), "tp")
    return jax.shard_map(
        local_block, mesh=mesh, in_specs=(row_spec, P("sp", "tp"), P("sp", "tp"), P(("dp", "sp"))),
        out_specs=row_spec, check_vma=False)
```

```python
import functools

import jax
import jax.numpy as jnp
from jax import lax
from jax.experimental import pallas as pl
from jax.experimental.pallas import tpu as pltpu
from jax.sharding import PartitionSpec as P

HEAD_DIM = 128
MESH = pl.DeviceIdType.MESH
ANY = pl.ANY
VMEM_LIMIT = 67_043_328


class Place:
    def __init__(self, n_tp, n_sp):
        self.n_tp, self.n_sp, self.n_x = n_tp, n_sp, n_sp // 2
        self.tp, self.sp = lax.axis_index("tp"), lax.axis_index("sp")
        self.chip, self.core = self.sp // 2, self.sp % 2
        self.sib = self.chip * 2 + 1 - self.core
        self.up, self.down = (self.tp + 1) % n_tp, (self.tp + n_tp - 1) % n_tp
        self.right, self.left = self.at(1, 0), self.at(-1, 0)

    def chip_at(self, r):
        return (self.chip + r + self.n_x) % self.n_x

    def at(self, r, d):
        return self.chip_at(r) * 2 + (self.core if d == 0 else 1 - self.core)

    def barrier(self):
        sem = pltpu.get_barrier_semaphore()
        for j in range(1, self.n_sp):
            pl.semaphore_signal(sem, inc=1, device_id={"sp": (self.sp + j) % self.n_sp}, device_id_type=MESH)
        for peer in (self.up, self.down):
            pl.semaphore_signal(sem, inc=1, device_id={"tp": peer}, device_id_type=MESH)
        pl.semaphore_wait(sem, self.n_sp + 1)


def remote(src, dst, send, recv, **peer):
    return pltpu.make_async_remote_copy(
        src_ref=src, dst_ref=dst, send_sem=send, recv_sem=recv, device_id=peer, device_id_type=MESH
    )


class Ring:
    HALF = (0, 1, 0, 1, 0, 1)

    def __init__(self, axis, me, ahead, behind, far, own, slots, rows, send, recv):
        self.half = (pl.ds(0, rows // 2), pl.ds(rows // 2, rows // 2))
        self.axis, self.me, self.ahead, self.behind, self.far = axis, me, ahead, behind, far
        self.own, self.slots, self.send, self.recv = own, slots, send, recv

    def copy(self, k):
        h = self.half[self.HALF[k]]
        if k in (2, 5):
            src = dst = self.landed(k - 2)
        else:
            src, dst = self.own.at[h], self.slots(self.me).at[h]
        peer = self.ahead if k < 3 else self.behind
        return remote(src, dst, self.send.at[k], self.recv.at[k], **{self.axis: peer})

    def landed(self, k):
        origin = (self.behind, self.behind, self.far, self.ahead, self.ahead, self.far)[k]
        return self.slots(origin).at[self.half[self.HALF[k]]]

    def start(self, *ks):
        for k in ks or (0, 3, 1, 4):
            self.copy(k).start()

    def forward(self):
        for k in (0, 3):
            self.copy(k).wait_recv()
            self.copy(k + 2).start()

    def wait(self, *ks):
        for k in ks:
            self.copy(k).wait_recv()

    def drain(self):
        for k in range(6):
            self.copy(k).wait_send()


class WeightGather:
    def __init__(self, p, own, slots, rows, send, recv, sib_send, sib_recv):
        self.p, self.send, self.recv = p, sib_send, sib_recv
        self.ring = Ring("sp", p.sp, p.right, p.left, p.at(2, 0), own, slots, rows, send, recv)
        self.own = remote(own, slots(p.sp), sib_send.at[6], sib_recv.at[6], sp=p.sib)

    def to_sibling(self, k):
        block = self.ring.landed(k)
        return remote(block, block, self.send.at[k], self.recv.at[k], sp=self.p.sib)

    def forward(self):
        self.ring.forward()
        self.share(0, 3)

    def share(self, *ks):
        for k in ks:
            self.to_sibling(k).start()

    def wait_sibling(self, *ks):
        for k in ks:
            self.to_sibling(k).wait_recv()

    def drain(self):
        self.ring.drain()
        self.own.wait_send()
        for k in range(6):
            self.to_sibling(k).wait_send()


LOWEST = -0.7 * 3.4028235e38
APART = 1e38


def attend(coef, q, keys, values_t, row0, last, scores, exps, probs, tops):
    q_tile = q.shape[0]
    k_tile = scores.shape[0]
    lanes = slice(0, q_tile)

    def score(j):
        scores[:, lanes] = lax.dot_general(keys(j), q, (((1,), (1,)), ((), ())), preferred_element_type=jnp.float32)

    def body(edge, j, carry):
        top, total = carry
        s = scores[:, lanes]
        if not edge:
            score(j + 1)
        else:
            key = j * k_tile + lax.broadcasted_iota(jnp.int32, s.shape, 0)
            row = row0 + lax.broadcasted_iota(jnp.int32, s.shape, 1)
            s = jnp.where(key <= row, s, LOWEST)
        new = jnp.maximum(top, jnp.max(s, axis=0, keepdims=True))
        e = jnp.exp2((s - new) * coef)
        exps[j, :, lanes] = e
        tops[j, :, lanes] = new
        total = total * jnp.exp2((top - new) * coef) + jnp.sum(e, axis=0, keepdims=True)
        return new, total

    carry = (jnp.full((1, q_tile), LOWEST, jnp.float32), jnp.zeros((1, q_tile), jnp.float32))
    score(0)
    carry = lax.fori_loop(0, last, functools.partial(body, False), carry)
    top, total = body(True, last, carry)
    inverse = 1.0 / total

    def prob(j):
        share = jnp.exp2((tops[j, :, lanes] - top) * coef) * inverse
        return (exps[j, :, lanes] * share).astype(jnp.bfloat16)

    def weigh(j, o):
        p = probs[:, lanes]
        probs[:, lanes] = prob(j + 1)
        return o + jnp.dot(values_t[j], p, preferred_element_type=jnp.float32)

    probs[:, lanes] = prob(0)
    o = lax.fori_loop(0, last, weigh, jnp.zeros((HEAD_DIM, q_tile), jnp.float32))
    return o + jnp.dot(values_t[last], probs[:, lanes], preferred_element_type=jnp.float32)


def beside_docs(q, docs):
    return jnp.concatenate([q, ((docs.astype(jnp.float32) - 1.0) * APART).astype(q.dtype)], axis=1)


def qkv_kernel(n_tp, n_sp, coef, x_ref, w_ref, seg_ref, o_out, docs_out, skv, sq, w_all,
               x_all, acc, qkv, w_tile, seg_all, m_all, values_t, docs, o_all, scores, exps, probs, tops,
               local_sem, tile_sem, x_send, x_recv, w_send, w_recv, w_sib_send, w_sib_recv, seg_send, seg_recv,
               main_send, main_recv, kv_send, kv_recv, q_send, q_recv, own_sem, o_sem):
    p = Place(n_tp, n_sp)
    rows, x_cols = x_ref.shape
    w_rows = w_ref.shape[0]
    n_main, _, tile = acc.shape
    n_tiles = n_main + 1
    head = 3 * HEAD_DIM
    n_shared = 2 * n_tiles - n_sp
    parts = n_sp // n_shared
    q_rows = rows // parts
    m_tile = min(rows, 256)
    n_keys, k_tile, q_tile = exps.shape
    seq = n_sp * rows
    n_docs = 4
    p.barrier()

    x_own = pltpu.make_async_copy(x_ref, x_all.at[p.tp], local_sem.at[0])
    x_own.start()
    seg_own = pltpu.make_async_copy(seg_ref, seg_all.at[p.sp], local_sem.at[1])
    seg_own.start()
    x_ring = Ring("tp", p.tp, p.up, p.down, (p.tp + 2) % n_tp, x_ref, lambda i: x_all.at[i], rows, x_send, x_recv)

    def gather(g):
        c = pl.ds(0, n_main * tile) if g == 0 else pl.ds(n_main * tile, tile)
        return WeightGather(p, w_ref.at[:, c], lambda i: w_all.at[i, :, c], w_rows, w_send.at[g], w_recv.at[g],
                            w_sib_send.at[g], w_sib_recv.at[g])

    mains, shared = gather(0), gather(1)
    mains.ring.start()
    x_ring.start()
    mains.own.start()
    shared.own.start()
    seg_copies = []
    for j in range(1, n_sp):
        copy = remote(seg_ref, seg_all.at[p.sp], seg_send.at[j - 1], seg_recv.at[j - 1], sp=(p.sp + j) % n_sp)
        copy.start()
        seg_copies.append(copy)

    def tile_load(w_src, t, slot):
        return pltpu.make_async_copy(
            w_src.at[:, pl.ds(pl.multiple_of(t * tile, tile), tile)], w_tile.at[slot], tile_sem.at[slot])

    def product(shard, m, slot):
        r = pl.ds(pl.multiple_of(m * m_tile, m_tile), m_tile)
        c = pl.ds(pl.multiple_of((shard % 2) * w_rows, w_rows), w_rows)
        return r, jnp.dot(x_all[shard // 2, r, c], w_tile[slot], preferred_element_type=jnp.float32)

    def source(shard, own=False):
        return w_ref if own else w_all.at[shard]

    def accumulate(w_src, shard, first=False):
        tile_load(w_src, 0, 0).start()

        @pl.loop(0, n_main)
        def _(t):
            slot = t % 2
            tile_load(w_src, t, slot).wait()

            @pl.when(t + 1 < n_main)
            def _():
                tile_load(w_src, t + 1, 1 - slot).start()

            @pl.loop(0, rows // m_tile)
            def _(m):
                r, d = product(shard, m, slot)
                if first:
                    acc[t, r] = d
                else:
                    acc[t, r] += d

    x_ring.forward()
    mains.forward()
    x_ring.wait(1, 4, 2, 5)
    mains.ring.wait(1, 4)
    mains.share(1, 4)
    x_own.wait()
    accumulate(w_ref, p.sp, first=True)
    mains.own.wait_recv()
    accumulate(w_all.at[p.sib], p.sib)
    accumulate(w_all.at[p.left], p.left)
    accumulate(w_all.at[p.right], p.right)
    mains.wait_sibling(0, 1)
    accumulate(w_all.at[p.at(-1, 1)], p.at(-1, 1))
    mains.wait_sibling(3, 4)
    accumulate(w_all.at[p.at(1, 1)], p.at(1, 1))
    shared.ring.start(0, 3)
    mains.ring.wait(2, 5)
    mains.share(2, 5)
    accumulate(w_all.at[p.at(2, 0)], p.at(2, 0))
    mains.wait_sibling(2, 5)

    last = p.at(2, 1)
    offsets = (2, 1, -1, 0)
    main_copies = []
    tile_load(w_all.at[last], p.chip_at(2), 0).start()
    for i, r in enumerate(offsets):
        t, slot = p.chip_at(r), i % 2
        tile_load(w_all.at[last], t, slot).wait()
        if i + 1 < n_main:
            tile_load(w_all.at[last], p.chip_at(offsets[i + 1]), 1 - slot).start()

        @pl.loop(0, rows // m_tile)
        def _(m):
            rr, d = product(last, m, slot)
            qkv[t, rr] = (acc[t, rr] + d).astype(qkv.dtype)

        for d in (0, 1):
            core = p.core if d == 0 else 1 - p.core
            src = qkv.at[t, :, pl.ds(pl.multiple_of(core * head, head), head)]
            if r == 0 and d == 0:
                copy = pltpu.make_async_copy(src, m_all.at[p.sp], own_sem.at[0])
            else:
                j = (r % 4) * 2 + d
                copy = remote(src, m_all.at[p.sp], main_send.at[j], main_recv.at[j], sp=p.at(r, d))
            copy.start()
            main_copies.append((copy, r == 0 and d == 0))

    shared.ring.start(1, 4)
    shared.forward()

    def accumulate_shared(a, b, a_own=False, step=0):
        for slot, (shard, own) in enumerate(((a, a_own), (b, False))):
            tile_load(source(shard, own), n_main, slot).start()
        for slot, (shard, own) in enumerate(((a, a_own), (b, False))):
            tile_load(source(shard, own), n_main, slot).wait()

        @pl.loop(0, rows // m_tile)
        def _(m):
            r, d = product(a, m, 0)
            d += product(b, m, 1)[1]
            if step == 0:
                acc[0, r] = d
            elif step == 1:
                acc[0, r] += d
            else:
                qkv[n_main, r] = (acc[0, r] + d).astype(qkv.dtype)

    shared.own.wait_recv()
    accumulate_shared(p.sp, p.sib, a_own=True)

    for copy in seg_copies:
        copy.wait()
    seg_own.wait()
    seg = seg_all[...]
    lane = lax.broadcasted_iota(jnp.int32, (1, HEAD_DIM), 1)
    begin = jnp.zeros((1, HEAD_DIM), jnp.float32)
    end = jnp.where(lane == n_docs - 1, jnp.float32(seq), 0.0)
    for d in range(1, n_docs):
        below = jnp.sum(jnp.where(seg < d, 1.0, 0.0), axis=0)
        below = jnp.sum(jnp.sum(below, axis=0, keepdims=True), axis=1, keepdims=True)
        begin += jnp.where(lane == d, below, 0.0)
        end += jnp.where(lane == d - 1, below, 0.0)

    @pl.loop(0, n_keys)
    def _(j):
        row = (j * k_tile + lax.broadcasted_iota(jnp.int32, (k_tile, HEAD_DIM), 0)).astype(jnp.float32)
        docs[j] = jnp.where((row >= begin) & (row < end), 1.0, 0.0).astype(docs.dtype)

    docs_copy = pltpu.make_async_copy(docs, docs_out, own_sem.at[3])
    docs_copy.start()

    for copy, local in main_copies:
        if local:
            copy.wait()
        else:
            copy.wait_recv()
    per = rows // k_tile

    @pl.loop(0, n_keys)
    def _(j):
        r = pl.ds(pl.multiple_of((j % per) * k_tile, k_tile), k_tile)
        values_t[j] = m_all[j // per, r, 2 * HEAD_DIM:].T

    def keys(j):
        r = pl.ds(pl.multiple_of((j % per) * k_tile, k_tile), k_tile)
        return jnp.concatenate([m_all[j // per, r, HEAD_DIM:2 * HEAD_DIM], docs[j]], axis=1)

    def o_copy(i):
        r = pl.ds(pl.multiple_of(i * q_tile, q_tile), q_tile)
        return pltpu.make_async_copy(o_all.at[r], o_out.at[r], o_sem.at[i])

    def main_attention(lo, hi):
        @pl.loop(lo, hi)
        def _(i):
            r = pl.ds(pl.multiple_of((i % per) * k_tile, k_tile), k_tile)
            q = beside_docs(m_all[i // per, r, :HEAD_DIM], docs[i])
            o = attend(coef, q, keys, values_t, i * q_tile, i, scores, exps, probs, tops)
            o_all[pl.ds(pl.multiple_of(i * q_tile, q_tile), q_tile)] = o.T.astype(o_all.dtype)
            o_copy(i).start()

    early = n_keys - 3
    main_attention(early, n_keys)

    shared.ring.wait(1, 4, 2, 5)
    shared.share(1, 4, 2, 5)
    shared.wait_sibling(0, 1)
    accumulate_shared(p.left, p.at(-1, 1), step=1)
    shared.wait_sibling(3, 4)
    accumulate_shared(p.right, p.at(1, 1), step=1)
    shared.wait_sibling(2, 5)
    accumulate_shared(p.at(2, 0), p.at(2, 1), step=2)

    shared_copies = []
    t = n_main
    for r in (2, 1, -1, 0):
        base = (p.chip_at(r) * 2 // parts) * head
        kv_src = qkv.at[t, :, pl.ds(pl.multiple_of(base + HEAD_DIM, HEAD_DIM), 2 * HEAD_DIM)]
        k = r % 4
        if r == 0:
            copy = pltpu.make_async_copy(kv_src, skv.at[p.sp], own_sem.at[1])
            copy.start()
            shared_copies.append((copy, True))
        copy = remote(kv_src, skv.at[p.sp], kv_send.at[k], kv_recv.at[k], sp=p.sib if r == 0 else p.at(r, 0))
        copy.start()
        shared_copies.append((copy, False if r == 0 else None))
        for d in (0, 1):
            dst = p.at(r, d)
            q_src = qkv.at[t, pl.ds(pl.multiple_of((dst % parts) * q_rows, q_rows), q_rows),
                           pl.ds(pl.multiple_of(base, HEAD_DIM), HEAD_DIM)]
            if r == 0 and d == 0:
                copy = pltpu.make_async_copy(q_src, sq.at[p.sp], own_sem.at[2])
            else:
                j = k * 2 + d
                copy = remote(q_src, sq.at[p.sp], q_send.at[j], q_recv.at[j], sp=dst)
            copy.start()
            shared_copies.append((copy, r == 0 and d == 0))

    main_attention(0, early)

    relays = []
    for r in (1, -1, 2):
        k = r % 4
        arrived = skv.at[p.at(-r, 0)]
        remote(arrived, arrived, kv_send.at[k], kv_recv.at[k], sp=p.at(r, 0)).wait_recv()
        relay = remote(arrived, arrived, kv_send.at[3 + k], kv_recv.at[3 + k], sp=p.sib)
        relay.start()
        relays.append(relay)
    for copy, local in shared_copies:
        if local:
            copy.wait()
        else:
            copy.wait_send()
            if local is False:
                copy.wait_recv()
    for relay in relays:
        relay.wait()
    for copy, local in main_copies:
        if not local:
            copy.wait_send()
    for i in range(n_keys):
        o_copy(i).wait()
    docs_copy.wait()
    x_ring.drain()
    mains.drain()
    shared.drain()


def out_kernel(n_tp, n_sp, coef, o_ref, docs_ref, skv_ref, sq_ref, w_ref, y_ref, ctx, w_all, acc, skv, sq, docs,
               values_t, so_all, scores, exps, probs, tops, local_sem, w_send, w_recv, w_sib_send, w_sib_recv,
               o_send, o_recv, s_send, s_recv, c_send, c_recv):
    p = Place(n_tp, n_sp)
    n_x = p.n_x
    _, rows, local = ctx.shape
    w_rows = w_ref.shape[0]
    n_shared = local // HEAD_DIM - n_sp
    parts = n_sp // n_shared
    q_rows = rows // parts
    m_tile = min(rows, 256)
    pair = 2 * HEAD_DIM
    n_keys, k_tile, _ = exps.shape
    per = rows // k_tile

    loads = [pltpu.make_async_copy(src, dst, local_sem.at[3 + i])
             for i, (src, dst) in enumerate(((skv_ref, skv), (sq_ref, sq), (docs_ref, docs)))]
    for load in loads:
        load.start()
    w_own = pltpu.make_async_copy(w_ref, w_all.at[p.sp], local_sem.at[0])
    w_own.start()
    p.barrier()

    def head_copy(r, d):
        dst = p.at(r, d)
        src = o_ref.at[pl.ds(pl.multiple_of(dst * rows, rows), rows)]
        to = ctx.at[p.tp, :, pl.ds(pl.multiple_of(p.sp * HEAD_DIM, HEAD_DIM), HEAD_DIM)]
        if r == 0 and d == 0:
            return pltpu.make_async_copy(src, to, local_sem.at[1])
        j = (r % 4) * 2 + d
        return remote(src, to, o_send.at[j], o_recv.at[j], sp=dst)

    def shared_copy(r, d):
        dst = p.at(r, d)
        src = so_all.at[pl.ds(pl.multiple_of(dst * q_rows, q_rows), q_rows)]
        to = ctx.at[p.tp, pl.ds(pl.multiple_of((p.sp % parts) * q_rows, q_rows), q_rows),
                    pl.ds(pl.multiple_of((n_sp + p.sp // parts) * HEAD_DIM, HEAD_DIM), HEAD_DIM)]
        if r == 0 and d == 0:
            return pltpu.make_async_copy(src, to, local_sem.at[2])
        j = (r % 4) * 2 + d
        return remote(src, to, s_send.at[j], s_recv.at[j], sp=dst)

    peers = [(r, d) for r in (0, 1, -1, 2) for d in (0, 1)]
    for r, d in peers:
        head_copy(r, d).start()
    weight = WeightGather(p, w_ref, lambda i: w_all.at[i], w_rows, w_send, w_recv, w_sib_send, w_sib_recv)
    weight.ring.start(0, 3)
    weight.own.start()

    def ring(i, column):
        c = pl.ds(pl.multiple_of(column, pair), pair)
        return Ring("tp", p.tp, p.up, p.down, (p.tp + 2) % n_tp, ctx.at[p.tp, :, c], lambda j: ctx.at[j, :, c], rows,
                    c_send.at[i], c_recv.at[i])

    def wait_in(copy, local):
        if local:
            copy.wait()
        else:
            copy.wait_recv()

    rings = []

    def start_ring(i, r):
        for d in (0, 1):
            wait_in(head_copy(r, d), r == 0 and d == 0)
        rings.append(ring(i, p.chip_at(-r) * pair))
        rings[-1].start()

    def keys(j):
        r = pl.ds(pl.multiple_of((j % per) * k_tile, k_tile), k_tile)
        return jnp.concatenate([skv[j // per, r, :HEAD_DIM], docs[j]], axis=1)

    def shared_attention(lo, hi):
        @pl.loop(lo, hi)
        def _(i):
            row0 = (i * parts + p.sp % parts) * q_rows
            j = row0 // k_tile
            r = pl.ds(pl.multiple_of(row0 % k_tile, q_rows), q_rows)
            q = beside_docs(sq[i], docs[j, r])
            o = attend(coef, q, keys, values_t, row0, j, scores, exps, probs, tops)
            so_all[pl.ds(pl.multiple_of(i * q_rows, q_rows), q_rows)] = o.T.astype(so_all.dtype)

    start_ring(0, 0)
    for load in loads:
        load.wait()

    @pl.loop(0, n_keys)
    def _(j):
        r = pl.ds(pl.multiple_of((j % per) * k_tile, k_tile), k_tile)
        values_t[j] = skv[j // per, r, HEAD_DIM:].T

    shared_attention(0, n_sp // 2)
    start_ring(1, 1)
    start_ring(2, -1)
    shared_attention(n_sp // 2, n_sp)
    for r, d in peers:
        shared_copy(r, d).start()
    weight.ring.start(1, 4)
    start_ring(3, 2)
    rings[0].forward()
    rings[1].forward()
    rings[2].forward()
    weight.forward()
    for r, d in peers:
        wait_in(shared_copy(r, d), r == 0 and d == 0)
    rings.append(ring(n_x, n_sp * HEAD_DIM))
    rings[-1].start()
    for c in rings[3:]:
        c.forward()
    weight.ring.wait(1, 4)
    weight.share(1, 4)
    for c in rings:
        c.wait(1, 4)
    w_own.wait()
    weight.own.wait_recv()
    weight.wait_sibling(0, 1, 3, 4)

    def block(j, step):
        @pl.loop(0, rows // m_tile)
        def _(m):
            r = pl.ds(pl.multiple_of(m * m_tile, m_tile), m_tile)
            d = jnp.dot(ctx[j, r, :w_rows], w_all[2 * j], preferred_element_type=jnp.float32)
            d += jnp.dot(ctx[j, r, w_rows:], w_all[2 * j + 1], preferred_element_type=jnp.float32)
            if step == 0:
                acc[r] = d
            elif step < n_tp - 1:
                acc[r] += d
            else:
                y_ref[r] = (acc[r] + d).astype(y_ref.dtype)

    turn = (p.chip + n_x - p.tp) % n_x
    far = turn // 2
    block((p.tp + far * (1 - turn % 2)) % n_tp, 0)
    block((p.tp + 1 + 2 * far) % n_tp, 1)
    weight.ring.wait(2, 5)
    weight.share(2, 5)
    weight.wait_sibling(2, 5)
    block((p.tp + far * (turn - 2) + (1 - far) * 3) % n_tp, 2)
    for c in rings:
        c.wait(2, 5)
    block((p.tp + 2) % n_tp, 3)

    for c in rings:
        c.drain()
    weight.drain()
    for r, d in peers:
        if not (r == 0 and d == 0):
            head_copy(r, d).wait_send()
            shared_copy(r, d).wait_send()


def solution(mesh):
    n_tp, n_sp = mesh.shape["tp"], mesh.shape["sp"]
    dma = pltpu.SemaphoreType.DMA
    hbm = pl.BlockSpec(memory_space=ANY)
    coef = 1.0 / HEAD_DIM ** 0.5 * 1.4426950408889634

    def params(collective_id):
        return pltpu.CompilerParams(collective_id=collective_id, has_side_effects=True, vmem_limit_bytes=VMEM_LIMIT)

    def local_block(x_blk, wqkv_blk, wout_blk, seg_blk):
        rows, x_cols = x_blk.shape
        w_rows, n_cols = wqkv_blk.shape
        head = 3 * HEAD_DIM
        heads = n_cols // head
        local = heads * HEAD_DIM
        parts = n_sp // (heads - n_sp)
        q_rows = rows // parts
        tile = 2 * head
        n_tiles = n_cols // tile
        n_main = n_tiles - 1
        seq = n_sp * rows
        q_tile = k_tile = 2 * q_rows
        n_keys = seq // k_tile
        bf16, f32 = x_blk.dtype, jnp.float32
        seg = seg_blk.reshape(rows // 128, 128)

        def attention_scratch(q):
            return [
                pltpu.VMEM((k_tile, q), f32),
                pltpu.VMEM((n_keys, k_tile, q), f32),
                pltpu.VMEM((k_tile, q), bf16),
                pltpu.VMEM((n_keys, 1, q), f32),
            ]

        o_main, docs, skv, sq, _ = pl.pallas_call(
            functools.partial(qkv_kernel, n_tp, n_sp, coef),
            out_shape=(
                jax.ShapeDtypeStruct((seq, HEAD_DIM), bf16),
                jax.ShapeDtypeStruct((n_keys, k_tile, HEAD_DIM), bf16),
                jax.ShapeDtypeStruct((n_sp, rows, 2 * HEAD_DIM), bf16),
                jax.ShapeDtypeStruct((n_sp, q_rows, HEAD_DIM), bf16),
                jax.ShapeDtypeStruct((n_sp, w_rows, n_cols), bf16),
            ),
            in_specs=[hbm] * 3,
            out_specs=(hbm,) * 5,
            scratch_shapes=[
                pltpu.VMEM((n_tp, rows, x_cols), bf16),
                pltpu.VMEM((n_main, rows, tile), f32),
                pltpu.VMEM((n_tiles, rows, tile), bf16),
                pltpu.VMEM((2, w_rows, tile), bf16),
                pltpu.VMEM((n_sp,) + seg.shape, seg.dtype),
                pltpu.VMEM((n_sp, rows, head), bf16),
                pltpu.VMEM((n_keys, HEAD_DIM, k_tile), bf16),
                pltpu.VMEM((n_keys, k_tile, HEAD_DIM), bf16),
                pltpu.VMEM((seq, HEAD_DIM), bf16),
                *attention_scratch(q_tile),
                dma((2,)), dma((2,)), dma((6,)), dma((6,)), dma((2, 6)), dma((2, 6)), dma((2, 7)), dma((2, 7)),
                dma((n_sp - 1,)), dma((n_sp - 1,)), dma((8,)), dma((8,)), dma((7,)), dma((7,)), dma((8,)), dma((8,)),
                dma((4,)), dma((n_keys,)),
            ],
            compiler_params=params(0),
            name="qkv",
        )(x_blk, wqkv_blk, seg)

        wo_rows, wo_cols = wout_blk.shape
        n_rings = local // (2 * HEAD_DIM)
        return pl.pallas_call(
            functools.partial(out_kernel, n_tp, n_sp, coef),
            out_shape=jax.ShapeDtypeStruct((rows, wo_cols), bf16),
            in_specs=[hbm] * 5,
            out_specs=pl.BlockSpec(memory_space=pltpu.VMEM),
            scratch_shapes=[
                pltpu.VMEM((n_tp, rows, local), bf16),
                pltpu.VMEM((n_sp, wo_rows, wo_cols), bf16),
                pltpu.VMEM((rows, wo_cols), f32),
                pltpu.VMEM((n_sp, rows, 2 * HEAD_DIM), bf16),
                pltpu.VMEM((n_sp, q_rows, HEAD_DIM), bf16),
                pltpu.VMEM((n_keys, k_tile, HEAD_DIM), bf16),
                pltpu.VMEM((n_keys, HEAD_DIM, k_tile), bf16),
                pltpu.VMEM((seq // parts, HEAD_DIM), bf16),
                *attention_scratch(q_rows),
                dma((6,)), dma((6,)), dma((6,)), dma((7,)), dma((7,)),
                dma((8,)), dma((8,)), dma((8,)), dma((8,)), dma((n_rings, 6)), dma((n_rings, 6)),
            ],
            compiler_params=params(1),
            name="out",
        )(o_main, docs, skv, sq, wout_blk)

    row_spec = P(("dp", "sp"), "tp")
    return jax.shard_map(
        local_block, mesh=mesh, in_specs=(row_spec, P("sp", "tp"), P("sp", "tp"), P(("dp", "sp"))),
        out_specs=row_spec, check_vma=False)
```

```python
import functools

import jax
import jax.numpy as jnp
from jax import lax
from jax.experimental import pallas as pl
from jax.experimental.pallas import tpu as pltpu
from jax.sharding import PartitionSpec as P

HEAD_DIM = 128
MESH = pl.DeviceIdType.MESH
ANY = pl.ANY
VMEM_LIMIT = 67_043_328


class Place:
    def __init__(self, n_tp, n_sp):
        self.n_tp, self.n_sp, self.n_x = n_tp, n_sp, n_sp // 2
        self.tp, self.sp = lax.axis_index("tp"), lax.axis_index("sp")
        self.chip, self.core = self.sp // 2, self.sp % 2
        self.sib = self.chip * 2 + 1 - self.core
        self.up, self.down = (self.tp + 1) % n_tp, (self.tp + n_tp - 1) % n_tp
        self.right, self.left = self.at(1, 0), self.at(-1, 0)

    def chip_at(self, r):
        return (self.chip + r + self.n_x) % self.n_x

    def at(self, r, d):
        return self.chip_at(r) * 2 + (self.core if d == 0 else 1 - self.core)

    def barrier(self):
        sem = pltpu.get_barrier_semaphore()
        for j in range(1, self.n_sp):
            pl.semaphore_signal(sem, inc=1, device_id={"sp": (self.sp + j) % self.n_sp}, device_id_type=MESH)
        for peer in (self.up, self.down):
            pl.semaphore_signal(sem, inc=1, device_id={"tp": peer}, device_id_type=MESH)
        pl.semaphore_wait(sem, self.n_sp + 1)


def remote(src, dst, send, recv, **peer):
    return pltpu.make_async_remote_copy(
        src_ref=src, dst_ref=dst, send_sem=send, recv_sem=recv, device_id=peer, device_id_type=MESH
    )


class Ring:
    HALF = (0, 1, 0, 1, 0, 1)

    def __init__(self, axis, me, ahead, behind, far, own, slots, rows, send, recv):
        self.half = (pl.ds(0, rows // 2), pl.ds(rows // 2, rows // 2))
        self.axis, self.me, self.ahead, self.behind, self.far = axis, me, ahead, behind, far
        self.own, self.slots, self.send, self.recv = own, slots, send, recv

    def copy(self, k):
        h = self.half[self.HALF[k]]
        if k in (2, 5):
            src = dst = self.landed(k - 2)
        else:
            src, dst = self.own.at[h], self.slots(self.me).at[h]
        peer = self.ahead if k < 3 else self.behind
        return remote(src, dst, self.send.at[k], self.recv.at[k], **{self.axis: peer})

    def landed(self, k):
        origin = (self.behind, self.behind, self.far, self.ahead, self.ahead, self.far)[k]
        return self.slots(origin).at[self.half[self.HALF[k]]]

    def start(self, *ks):
        for k in ks or (0, 3, 1, 4):
            self.copy(k).start()

    def forward(self):
        for k in (0, 3):
            self.copy(k).wait_recv()
            self.copy(k + 2).start()

    def wait(self, *ks):
        for k in ks:
            self.copy(k).wait_recv()

    def drain(self):
        for k in range(6):
            self.copy(k).wait_send()


class WeightGather:
    def __init__(self, p, own, slots, rows, send, recv, sib_send, sib_recv):
        self.p, self.send, self.recv = p, sib_send, sib_recv
        self.ring = Ring("sp", p.sp, p.right, p.left, p.at(2, 0), own, slots, rows, send, recv)
        self.own = remote(own, slots(p.sp), sib_send.at[6], sib_recv.at[6], sp=p.sib)

    def to_sibling(self, k):
        block = self.ring.landed(k)
        return remote(block, block, self.send.at[k], self.recv.at[k], sp=self.p.sib)

    def forward(self):
        self.ring.forward()
        self.share(0, 3)

    def share(self, *ks):
        for k in ks:
            self.to_sibling(k).start()

    def wait_sibling(self, *ks):
        for k in ks:
            self.to_sibling(k).wait_recv()

    def drain(self):
        self.ring.drain()
        self.own.wait_send()
        for k in range(6):
            self.to_sibling(k).wait_send()


LOWEST = -0.7 * 3.4028235e38
APART = 1e38


def attend(coef, q, keys, values_t, row0, last, scores, exps, probs, tops):
    q_tile = q.shape[0]
    k_tile = scores.shape[0]
    lanes = slice(0, q_tile)

    def score(j):
        scores[:, lanes] = lax.dot_general(keys(j), q, (((1,), (1,)), ((), ())), preferred_element_type=jnp.float32)

    def body(edge, j, carry):
        top, total = carry
        s = scores[:, lanes]
        if not edge:
            score(j + 1)
        else:
            key = j * k_tile + lax.broadcasted_iota(jnp.int32, s.shape, 0)
            row = row0 + lax.broadcasted_iota(jnp.int32, s.shape, 1)
            s = jnp.where(key <= row, s, LOWEST)
        new = jnp.maximum(top, jnp.max(s, axis=0, keepdims=True))
        e = jnp.exp2((s - new) * coef)
        exps[j, :, lanes] = e
        tops[j, :, lanes] = new
        total = total * jnp.exp2((top - new) * coef) + jnp.sum(e, axis=0, keepdims=True)
        return new, total

    carry = (jnp.full((1, q_tile), LOWEST, jnp.float32), jnp.zeros((1, q_tile), jnp.float32))
    score(0)
    carry = lax.fori_loop(0, last, functools.partial(body, False), carry)
    top, total = body(True, last, carry)
    inverse = 1.0 / total

    def prob(j):
        share = jnp.exp2((tops[j, :, lanes] - top) * coef) * inverse
        return (exps[j, :, lanes] * share).astype(jnp.bfloat16)

    def weigh(j, o):
        p = probs[:, lanes]
        probs[:, lanes] = prob(j + 1)
        return o + jnp.dot(values_t[j], p, preferred_element_type=jnp.float32)

    probs[:, lanes] = prob(0)
    o = lax.fori_loop(0, last, weigh, jnp.zeros((HEAD_DIM, q_tile), jnp.float32))
    return o + jnp.dot(values_t[last], probs[:, lanes], preferred_element_type=jnp.float32)


def beside_docs(q, docs):
    return jnp.concatenate([q, ((docs.astype(jnp.float32) - 1.0) * APART).astype(q.dtype)], axis=1)


def qkv_kernel(n_tp, n_sp, coef, n_done, x_ref, w_ref, seg_ref, o_out, docs_out, m_out, seg_out, skv, sq, w_all,
               x_all, acc, qkv, w_tile, seg_all, m_all, values_t, docs, o_all, scores, exps, probs, tops,
               local_sem, tile_sem, x_send, x_recv, w_send, w_recv, w_sib_send, w_sib_recv, seg_send, seg_recv,
               main_send, main_recv, kv_send, kv_recv, q_send, q_recv, own_sem, o_sem):
    p = Place(n_tp, n_sp)
    rows, x_cols = x_ref.shape
    w_rows = w_ref.shape[0]
    n_main, _, tile = acc.shape
    n_tiles = n_main + 1
    head = 3 * HEAD_DIM
    n_shared = 2 * n_tiles - n_sp
    parts = n_sp // n_shared
    q_rows = rows // parts
    m_tile = min(rows, 256)
    n_keys, k_tile, q_tile = exps.shape
    seq = n_sp * rows
    n_docs = 4
    p.barrier()

    x_own = pltpu.make_async_copy(x_ref, x_all.at[p.tp], local_sem.at[0])
    x_own.start()
    seg_own = pltpu.make_async_copy(seg_ref, seg_all.at[p.sp], local_sem.at[1])
    seg_own.start()
    x_ring = Ring("tp", p.tp, p.up, p.down, (p.tp + 2) % n_tp, x_ref, lambda i: x_all.at[i], rows, x_send, x_recv)

    def gather(g):
        c = pl.ds(0, n_main * tile) if g == 0 else pl.ds(n_main * tile, tile)
        return WeightGather(p, w_ref.at[:, c], lambda i: w_all.at[i, :, c], w_rows, w_send.at[g], w_recv.at[g],
                            w_sib_send.at[g], w_sib_recv.at[g])

    mains, shared = gather(0), gather(1)
    mains.ring.start()
    x_ring.start()
    mains.own.start()
    shared.own.start()
    seg_copies = []
    for j in range(1, n_sp):
        copy = remote(seg_ref, seg_all.at[p.sp], seg_send.at[j - 1], seg_recv.at[j - 1], sp=(p.sp + j) % n_sp)
        copy.start()
        seg_copies.append(copy)

    def tile_load(w_src, t, slot):
        return pltpu.make_async_copy(
            w_src.at[:, pl.ds(pl.multiple_of(t * tile, tile), tile)], w_tile.at[slot], tile_sem.at[slot])

    def product(shard, m, slot):
        r = pl.ds(pl.multiple_of(m * m_tile, m_tile), m_tile)
        c = pl.ds(pl.multiple_of((shard % 2) * w_rows, w_rows), w_rows)
        return r, jnp.dot(x_all[shard // 2, r, c], w_tile[slot], preferred_element_type=jnp.float32)

    def source(shard, own=False):
        return w_ref if own else w_all.at[shard]

    def accumulate(w_src, shard, first=False):
        tile_load(w_src, 0, 0).start()

        @pl.loop(0, n_main)
        def _(t):
            slot = t % 2
            tile_load(w_src, t, slot).wait()

            @pl.when(t + 1 < n_main)
            def _():
                tile_load(w_src, t + 1, 1 - slot).start()

            @pl.loop(0, rows // m_tile)
            def _(m):
                r, d = product(shard, m, slot)
                if first:
                    acc[t, r] = d
                else:
                    acc[t, r] += d

    x_ring.forward()
    mains.forward()
    x_ring.wait(1, 4, 2, 5)
    mains.ring.wait(1, 4)
    mains.share(1, 4)
    x_own.wait()
    accumulate(w_ref, p.sp, first=True)
    mains.own.wait_recv()
    accumulate(w_all.at[p.sib], p.sib)
    accumulate(w_all.at[p.left], p.left)
    accumulate(w_all.at[p.right], p.right)
    mains.wait_sibling(0, 1)
    accumulate(w_all.at[p.at(-1, 1)], p.at(-1, 1))
    mains.wait_sibling(3, 4)
    accumulate(w_all.at[p.at(1, 1)], p.at(1, 1))
    shared.ring.start(0, 3)
    mains.ring.wait(2, 5)
    mains.share(2, 5)
    accumulate(w_all.at[p.at(2, 0)], p.at(2, 0))
    mains.wait_sibling(2, 5)

    last = p.at(2, 1)
    offsets = (2, 1, -1, 0)
    main_copies = []
    tile_load(w_all.at[last], p.chip_at(2), 0).start()
    for i, r in enumerate(offsets):
        t, slot = p.chip_at(r), i % 2
        tile_load(w_all.at[last], t, slot).wait()
        if i + 1 < n_main:
            tile_load(w_all.at[last], p.chip_at(offsets[i + 1]), 1 - slot).start()

        @pl.loop(0, rows // m_tile)
        def _(m):
            rr, d = product(last, m, slot)
            qkv[t, rr] = (acc[t, rr] + d).astype(qkv.dtype)

        for d in (0, 1):
            core = p.core if d == 0 else 1 - p.core
            src = qkv.at[t, :, pl.ds(pl.multiple_of(core * head, head), head)]
            if r == 0 and d == 0:
                copy = pltpu.make_async_copy(src, m_all.at[p.sp], own_sem.at[0])
            else:
                j = (r % 4) * 2 + d
                copy = remote(src, m_all.at[p.sp], main_send.at[j], main_recv.at[j], sp=p.at(r, d))
            copy.start()
            main_copies.append((copy, r == 0 and d == 0))

    shared.ring.start(1, 4)
    shared.forward()

    def accumulate_shared(a, b, a_own=False, step=0):
        for slot, (shard, own) in enumerate(((a, a_own), (b, False))):
            tile_load(source(shard, own), n_main, slot).start()
        for slot, (shard, own) in enumerate(((a, a_own), (b, False))):
            tile_load(source(shard, own), n_main, slot).wait()

        @pl.loop(0, rows // m_tile)
        def _(m):
            r, d = product(a, m, 0)
            d += product(b, m, 1)[1]
            if step == 0:
                acc[0, r] = d
            elif step == 1:
                acc[0, r] += d
            else:
                qkv[n_main, r] = (acc[0, r] + d).astype(qkv.dtype)

    shared.own.wait_recv()
    accumulate_shared(p.sp, p.sib, a_own=True)

    for copy in seg_copies:
        copy.wait()
    seg_own.wait()
    seg = seg_all[...]
    lane = lax.broadcasted_iota(jnp.int32, (1, HEAD_DIM), 1)
    begin = jnp.zeros((1, HEAD_DIM), jnp.float32)
    end = jnp.where(lane == n_docs - 1, jnp.float32(seq), 0.0)
    for d in range(1, n_docs):
        below = jnp.sum(jnp.where(seg < d, 1.0, 0.0), axis=0)
        below = jnp.sum(jnp.sum(below, axis=0, keepdims=True), axis=1, keepdims=True)
        begin += jnp.where(lane == d, below, 0.0)
        end += jnp.where(lane == d - 1, below, 0.0)

    @pl.loop(0, n_keys)
    def _(j):
        row = (j * k_tile + lax.broadcasted_iota(jnp.int32, (k_tile, HEAD_DIM), 0)).astype(jnp.float32)
        docs[j] = jnp.where((row >= begin) & (row < end), 1.0, 0.0).astype(docs.dtype)

    docs_copy = pltpu.make_async_copy(docs, docs_out, own_sem.at[3])
    docs_copy.start()

    seg_copy = pltpu.make_async_copy(seg_all, seg_out, own_sem.at[4])
    seg_copy.start()

    for copy, local in main_copies:
        if local:
            copy.wait()
        else:
            copy.wait_recv()
    m_copy = pltpu.make_async_copy(m_all, m_out, own_sem.at[5])
    m_copy.start()
    per = rows // k_tile

    @pl.loop(0, n_keys)
    def _(j):
        r = pl.ds(pl.multiple_of((j % per) * k_tile, k_tile), k_tile)
        values_t[j] = m_all[j // per, r, 2 * HEAD_DIM:].T

    def keys(j):
        r = pl.ds(pl.multiple_of((j % per) * k_tile, k_tile), k_tile)
        return jnp.concatenate([m_all[j // per, r, HEAD_DIM:2 * HEAD_DIM], docs[j]], axis=1)

    def o_copy(i):
        r = pl.ds(pl.multiple_of(i * q_tile, q_tile), q_tile)
        return pltpu.make_async_copy(o_all.at[r], o_out.at[r], o_sem.at[i])

    def main_attention(lo, hi):
        @pl.loop(lo, hi)
        def _(i):
            r = pl.ds(pl.multiple_of((i % per) * k_tile, k_tile), k_tile)
            q = beside_docs(m_all[i // per, r, :HEAD_DIM], docs[i])
            o = attend(coef, q, keys, values_t, i * q_tile, i, scores, exps, probs, tops)
            o_all[pl.ds(pl.multiple_of(i * q_tile, q_tile), q_tile)] = o.T.astype(o_all.dtype)
            o_copy(i).start()

    early = n_done * 5 // 9
    main_attention(0, early)

    shared.ring.wait(1, 4, 2, 5)
    shared.share(1, 4, 2, 5)
    shared.wait_sibling(0, 1)
    accumulate_shared(p.left, p.at(-1, 1), step=1)
    shared.wait_sibling(3, 4)
    accumulate_shared(p.right, p.at(1, 1), step=1)
    shared.wait_sibling(2, 5)
    accumulate_shared(p.at(2, 0), p.at(2, 1), step=2)

    shared_copies = []
    t = n_main
    for r in (2, 1, -1, 0):
        base = (p.chip_at(r) * 2 // parts) * head
        kv_src = qkv.at[t, :, pl.ds(pl.multiple_of(base + HEAD_DIM, HEAD_DIM), 2 * HEAD_DIM)]
        k = r % 4
        if r == 0:
            copy = pltpu.make_async_copy(kv_src, skv.at[p.sp], own_sem.at[1])
            copy.start()
            shared_copies.append((copy, True))
        copy = remote(kv_src, skv.at[p.sp], kv_send.at[k], kv_recv.at[k], sp=p.sib if r == 0 else p.at(r, 0))
        copy.start()
        shared_copies.append((copy, False if r == 0 else None))
        for d in (0, 1):
            dst = p.at(r, d)
            q_src = qkv.at[t, pl.ds(pl.multiple_of((dst % parts) * q_rows, q_rows), q_rows),
                           pl.ds(pl.multiple_of(base, HEAD_DIM), HEAD_DIM)]
            if r == 0 and d == 0:
                copy = pltpu.make_async_copy(q_src, sq.at[p.sp], own_sem.at[2])
            else:
                j = k * 2 + d
                copy = remote(q_src, sq.at[p.sp], q_send.at[j], q_recv.at[j], sp=dst)
            copy.start()
            shared_copies.append((copy, r == 0 and d == 0))

    main_attention(early, n_done)

    relays = []
    for r in (1, -1, 2):
        k = r % 4
        arrived = skv.at[p.at(-r, 0)]
        remote(arrived, arrived, kv_send.at[k], kv_recv.at[k], sp=p.at(r, 0)).wait_recv()
        relay = remote(arrived, arrived, kv_send.at[3 + k], kv_recv.at[3 + k], sp=p.sib)
        relay.start()
        relays.append(relay)
    for copy, local in shared_copies:
        if local:
            copy.wait()
        else:
            copy.wait_send()
            if local is False:
                copy.wait_recv()
    for relay in relays:
        relay.wait()
    for copy, local in main_copies:
        if not local:
            copy.wait_send()
    for i in range(n_done):
        o_copy(i).wait()
    docs_copy.wait()
    seg_copy.wait()
    m_copy.wait()
    x_ring.drain()
    mains.drain()
    shared.drain()


def tail_kernel(coef, n_done, tab, m_ref, o_in, o_ref, vt, scores, exps, probs, tops):
    del o_in
    step = pl.program_id(0)
    seq = m_ref.shape[0]
    _, k_tile, _ = exps.shape
    n_bounds = tab.shape[0]

    @pl.when(step == 0)
    def _():
        @pl.loop(0, seq // k_tile)
        def _(j):
            r = pl.ds(pl.multiple_of(j * k_tile, k_tile), k_tile)
            vt[j] = m_ref[r, 2 * HEAD_DIM:].T

    def doc_start(row):
        start = row * 0
        for d in range(n_bounds):
            start = jnp.where(row >= tab[d], tab[d], start)
        return start

    def attend_tail(q, k_ref, k_col, vt_ref, row0, out):
        q_tile = q.shape[0]
        lanes = slice(0, q_tile)
        row = row0 + lax.broadcasted_iota(jnp.int32, (1, q_tile), 1)
        start = doc_start(row)
        first = doc_start(row0) // k_tile
        last = row0 // k_tile
        clear = (doc_start(row0 + q_tile - 1) + k_tile - 1) // k_tile
        clear = jnp.minimum(clear, last)

        def score(j):
            r = pl.ds(pl.multiple_of(j * k_tile, k_tile), k_tile)
            scores[:, lanes] = lax.dot_general(k_ref[r, k_col:k_col + HEAD_DIM], q, (((1,), (1,)), ((), ())),
                                               preferred_element_type=jnp.float32)

        def body(edge, j, carry):
            top, total = carry
            s = scores[:, lanes]
            if edge != "last":
                score(j + 1)
            if edge:
                key = j * k_tile + lax.broadcasted_iota(jnp.int32, s.shape, 0)
                seen = key >= start
                if edge == "last":
                    seen &= key <= row
                s = jnp.where(seen, s, LOWEST)
            new = jnp.maximum(top, jnp.max(s, axis=0, keepdims=True))
            e = jnp.exp2((s - new) * coef)
            exps[j, :, lanes] = e
            tops[j, :, lanes] = new
            total = total * jnp.exp2((top - new) * coef) + jnp.sum(e, axis=0, keepdims=True)
            return new, total

        carry = (jnp.full((1, q_tile), LOWEST, jnp.float32), jnp.zeros((1, q_tile), jnp.float32))
        score(first)
        carry = lax.fori_loop(first, clear, functools.partial(body, "first"), carry)
        carry = lax.fori_loop(clear, last, functools.partial(body, ""), carry)
        top, total = body("last", last, carry)
        inverse = 1.0 / total

        def prob(j):
            share = jnp.exp2((tops[j, :, lanes] - top) * coef) * inverse
            return (exps[j, :, lanes] * share).astype(jnp.bfloat16)

        def weigh(j, o):
            p = probs[:, lanes]
            probs[:, lanes] = prob(j + 1)
            return o + jnp.dot(vt_ref[j], p, preferred_element_type=jnp.float32)

        probs[:, lanes] = prob(first)
        o = lax.fori_loop(first, last, weigh, jnp.zeros((HEAD_DIM, q_tile), jnp.float32))
        o = o + jnp.dot(vt_ref[last], probs[:, lanes], preferred_element_type=jnp.float32)
        out[...] = o.T.astype(out.dtype)

    q_tile = o_ref.shape[0]
    row0 = (step + n_done) * q_tile
    q = m_ref[pl.ds(pl.multiple_of(row0, q_tile), q_tile), :HEAD_DIM]
    attend_tail(q, m_ref, HEAD_DIM, vt, row0, o_ref)


def out_kernel(n_tp, n_sp, coef, o_ref, docs_ref, skv_ref, sq_ref, w_ref, y_ref, ctx, w_all, acc, skv, sq, docs,
               values_t, so_all, scores, exps, probs, tops, local_sem, w_send, w_recv, w_sib_send, w_sib_recv,
               o_send, o_recv, s_send, s_recv, c_send, c_recv):
    p = Place(n_tp, n_sp)
    n_x = p.n_x
    _, rows, local = ctx.shape
    w_rows = w_ref.shape[0]
    n_shared = local // HEAD_DIM - n_sp
    parts = n_sp // n_shared
    q_rows = rows // parts
    m_tile = min(rows, 256)
    pair = 2 * HEAD_DIM
    n_keys, k_tile, _ = exps.shape
    per = rows // k_tile

    loads = [pltpu.make_async_copy(src, dst, local_sem.at[3 + i])
             for i, (src, dst) in enumerate(((skv_ref, skv), (sq_ref, sq), (docs_ref, docs)))]
    for load in loads:
        load.start()
    w_own = pltpu.make_async_copy(w_ref, w_all.at[p.sp], local_sem.at[0])
    w_own.start()
    p.barrier()

    def head_copy(r, d):
        dst = p.at(r, d)
        src = o_ref.at[pl.ds(pl.multiple_of(dst * rows, rows), rows)]
        to = ctx.at[p.tp, :, pl.ds(pl.multiple_of(p.sp * HEAD_DIM, HEAD_DIM), HEAD_DIM)]
        if r == 0 and d == 0:
            return pltpu.make_async_copy(src, to, local_sem.at[1])
        j = (r % 4) * 2 + d
        return remote(src, to, o_send.at[j], o_recv.at[j], sp=dst)

    def shared_copy(r, d):
        dst = p.at(r, d)
        src = so_all.at[pl.ds(pl.multiple_of(dst * q_rows, q_rows), q_rows)]
        to = ctx.at[p.tp, pl.ds(pl.multiple_of((p.sp % parts) * q_rows, q_rows), q_rows),
                    pl.ds(pl.multiple_of((n_sp + p.sp // parts) * HEAD_DIM, HEAD_DIM), HEAD_DIM)]
        if r == 0 and d == 0:
            return pltpu.make_async_copy(src, to, local_sem.at[2])
        j = (r % 4) * 2 + d
        return remote(src, to, s_send.at[j], s_recv.at[j], sp=dst)

    peers = [(r, d) for r in (0, 1, -1, 2) for d in (0, 1)]
    for r, d in peers:
        head_copy(r, d).start()
    weight = WeightGather(p, w_ref, lambda i: w_all.at[i], w_rows, w_send, w_recv, w_sib_send, w_sib_recv)
    weight.ring.start(0, 3)
    weight.own.start()

    def ring(i, column):
        c = pl.ds(pl.multiple_of(column, pair), pair)
        return Ring("tp", p.tp, p.up, p.down, (p.tp + 2) % n_tp, ctx.at[p.tp, :, c], lambda j: ctx.at[j, :, c], rows,
                    c_send.at[i], c_recv.at[i])

    def wait_in(copy, local):
        if local:
            copy.wait()
        else:
            copy.wait_recv()

    rings = []

    def start_ring(i, r):
        for d in (0, 1):
            wait_in(head_copy(r, d), r == 0 and d == 0)
        rings.append(ring(i, p.chip_at(-r) * pair))
        rings[-1].start()

    def keys(j):
        r = pl.ds(pl.multiple_of((j % per) * k_tile, k_tile), k_tile)
        return jnp.concatenate([skv[j // per, r, :HEAD_DIM], docs[j]], axis=1)

    def shared_attention(lo, hi):
        @pl.loop(lo, hi)
        def _(i):
            row0 = (i * parts + p.sp % parts) * q_rows
            j = row0 // k_tile
            r = pl.ds(pl.multiple_of(row0 % k_tile, q_rows), q_rows)
            q = beside_docs(sq[i], docs[j, r])
            o = attend(coef, q, keys, values_t, row0, j, scores, exps, probs, tops)
            so_all[pl.ds(pl.multiple_of(i * q_rows, q_rows), q_rows)] = o.T.astype(so_all.dtype)

    start_ring(0, 0)
    for load in loads:
        load.wait()

    @pl.loop(0, n_keys)
    def _(j):
        r = pl.ds(pl.multiple_of((j % per) * k_tile, k_tile), k_tile)
        values_t[j] = skv[j // per, r, HEAD_DIM:].T

    shared_attention(0, n_sp // 2)
    start_ring(1, 1)
    start_ring(2, -1)
    shared_attention(n_sp // 2, n_sp)
    for r, d in peers:
        shared_copy(r, d).start()
    weight.ring.start(1, 4)
    start_ring(3, 2)
    rings[0].forward()
    rings[1].forward()
    rings[2].forward()
    weight.forward()
    for r, d in peers:
        wait_in(shared_copy(r, d), r == 0 and d == 0)
    rings.append(ring(n_x, n_sp * HEAD_DIM))
    rings[-1].start()
    for c in rings[3:]:
        c.forward()
    weight.ring.wait(1, 4)
    weight.share(1, 4)
    for c in rings:
        c.wait(1, 4)
    w_own.wait()
    weight.own.wait_recv()
    weight.wait_sibling(0, 1, 3, 4)

    def block(j, step):
        @pl.loop(0, rows // m_tile)
        def _(m):
            r = pl.ds(pl.multiple_of(m * m_tile, m_tile), m_tile)
            d = jnp.dot(ctx[j, r, :w_rows], w_all[2 * j], preferred_element_type=jnp.float32)
            d += jnp.dot(ctx[j, r, w_rows:], w_all[2 * j + 1], preferred_element_type=jnp.float32)
            if step == 0:
                acc[r] = d
            elif step < n_tp - 1:
                acc[r] += d
            else:
                y_ref[r] = (acc[r] + d).astype(y_ref.dtype)

    turn = (p.chip + n_x - p.tp) % n_x
    far = turn // 2
    block((p.tp + far * (1 - turn % 2)) % n_tp, 0)
    block((p.tp + 1 + 2 * far) % n_tp, 1)
    weight.ring.wait(2, 5)
    weight.share(2, 5)
    weight.wait_sibling(2, 5)
    block((p.tp + far * (turn - 2) + (1 - far) * 3) % n_tp, 2)
    for c in rings:
        c.wait(2, 5)
    block((p.tp + 2) % n_tp, 3)

    for c in rings:
        c.drain()
    weight.drain()
    for r, d in peers:
        if not (r == 0 and d == 0):
            head_copy(r, d).wait_send()
            shared_copy(r, d).wait_send()


def solution(mesh):
    n_tp, n_sp = mesh.shape["tp"], mesh.shape["sp"]
    dma = pltpu.SemaphoreType.DMA
    hbm = pl.BlockSpec(memory_space=ANY)
    coef = 1.0 / HEAD_DIM ** 0.5 * 1.4426950408889634

    def params(collective_id):
        return pltpu.CompilerParams(collective_id=collective_id, has_side_effects=True, vmem_limit_bytes=VMEM_LIMIT)

    def local_block(x_blk, wqkv_blk, wout_blk, seg_blk):
        rows, x_cols = x_blk.shape
        w_rows, n_cols = wqkv_blk.shape
        head = 3 * HEAD_DIM
        heads = n_cols // head
        local = heads * HEAD_DIM
        parts = n_sp // (heads - n_sp)
        q_rows = rows // parts
        tile = 2 * head
        n_tiles = n_cols // tile
        n_main = n_tiles - 1
        seq = n_sp * rows
        q_tile = k_tile = 2 * q_rows
        n_keys = seq // k_tile
        bf16, f32 = x_blk.dtype, jnp.float32
        seg = seg_blk.reshape(rows // 128, 128)

        def attention_scratch(q):
            return [
                pltpu.VMEM((k_tile, q), f32),
                pltpu.VMEM((n_keys, k_tile, q), f32),
                pltpu.VMEM((k_tile, q), bf16),
                pltpu.VMEM((n_keys, 1, q), f32),
            ]

        n_done = n_keys * 9 // 16
        o_main, docs, m_all, seg_all, skv, sq, _ = pl.pallas_call(
            functools.partial(qkv_kernel, n_tp, n_sp, coef, n_done),
            out_shape=(
                jax.ShapeDtypeStruct((seq, HEAD_DIM), bf16),
                jax.ShapeDtypeStruct((n_keys, k_tile, HEAD_DIM), bf16),
                jax.ShapeDtypeStruct((n_sp, rows, head), bf16),
                jax.ShapeDtypeStruct((n_sp,) + seg.shape, seg.dtype),
                jax.ShapeDtypeStruct((n_sp, rows, 2 * HEAD_DIM), bf16),
                jax.ShapeDtypeStruct((n_sp, q_rows, HEAD_DIM), bf16),
                jax.ShapeDtypeStruct((n_sp, w_rows, n_cols), bf16),
            ),
            in_specs=[hbm] * 3,
            out_specs=(hbm,) * 7,
            scratch_shapes=[
                pltpu.VMEM((n_tp, rows, x_cols), bf16),
                pltpu.VMEM((n_main, rows, tile), f32),
                pltpu.VMEM((n_tiles, rows, tile), bf16),
                pltpu.VMEM((2, w_rows, tile), bf16),
                pltpu.VMEM((n_sp,) + seg.shape, seg.dtype),
                pltpu.VMEM((n_sp, rows, head), bf16),
                pltpu.VMEM((n_keys, HEAD_DIM, k_tile), bf16),
                pltpu.VMEM((n_keys, k_tile, HEAD_DIM), bf16),
                pltpu.VMEM((seq, HEAD_DIM), bf16),
                *attention_scratch(q_tile),
                dma((2,)), dma((2,)), dma((6,)), dma((6,)), dma((2, 6)), dma((2, 6)), dma((2, 7)), dma((2, 7)),
                dma((n_sp - 1,)), dma((n_sp - 1,)), dma((8,)), dma((8,)), dma((7,)), dma((7,)), dma((8,)), dma((8,)),
                dma((6,)), dma((n_keys,)),
            ],
            compiler_params=params(0),
            name="qkv",
        )(x_blk, wqkv_blk, seg)

        seg_ids = jnp.arange(1, 4, dtype=seg_all.dtype)[:, None]
        starts = jnp.sum((seg_all.reshape(1, seq) < seg_ids).astype(jnp.int32), axis=1)
        o_main = pl.pallas_call(
            functools.partial(tail_kernel, coef, n_done),
            out_shape=jax.ShapeDtypeStruct((seq, HEAD_DIM), bf16),
            grid_spec=pltpu.PrefetchScalarGridSpec(
                num_scalar_prefetch=1,
                grid=(n_keys - n_done,),
                in_specs=[pl.BlockSpec((seq, head), lambda i, t: (0, 0), pipeline_mode=pl.Buffered(1)), hbm],
                out_specs=pl.BlockSpec((q_tile, HEAD_DIM), lambda i, t: (i + n_done, 0)),
                scratch_shapes=[pltpu.VMEM((n_keys, HEAD_DIM, k_tile), bf16), *attention_scratch(q_tile)],
            ),
            input_output_aliases={2: 0},
            compiler_params=pltpu.CompilerParams(dimension_semantics=("arbitrary",), vmem_limit_bytes=VMEM_LIMIT),
            name="tail",
        )(starts, m_all.reshape(seq, head), o_main)

        wo_rows, wo_cols = wout_blk.shape
        n_rings = local // (2 * HEAD_DIM)
        return pl.pallas_call(
            functools.partial(out_kernel, n_tp, n_sp, coef),
            out_shape=jax.ShapeDtypeStruct((rows, wo_cols), bf16),
            in_specs=[hbm] * 5,
            out_specs=pl.BlockSpec(memory_space=pltpu.VMEM),
            scratch_shapes=[
                pltpu.VMEM((n_tp, rows, local), bf16),
                pltpu.VMEM((n_sp, wo_rows, wo_cols), bf16),
                pltpu.VMEM((rows, wo_cols), f32),
                pltpu.VMEM((n_sp, rows, 2 * HEAD_DIM), bf16),
                pltpu.VMEM((n_sp, q_rows, HEAD_DIM), bf16),
                pltpu.VMEM((n_keys, k_tile, HEAD_DIM), bf16),
                pltpu.VMEM((n_keys, HEAD_DIM, k_tile), bf16),
                pltpu.VMEM((seq // parts, HEAD_DIM), bf16),
                *attention_scratch(q_rows),
                dma((6,)), dma((6,)), dma((6,)), dma((7,)), dma((7,)),
                dma((8,)), dma((8,)), dma((8,)), dma((8,)), dma((n_rings, 6)), dma((n_rings, 6)),
            ],
            compiler_params=params(1),
            name="out",
        )(o_main, docs, skv, sq, wout_blk)

    row_spec = P(("dp", "sp"), "tp")
    return jax.shard_map(
        local_block, mesh=mesh, in_specs=(row_spec, P("sp", "tp"), P("sp", "tp"), P(("dp", "sp"))),
        out_specs=row_spec, check_vma=False)
```

```python
import functools

import jax
import jax.numpy as jnp
from jax import lax
from jax.experimental import pallas as pl
from jax.experimental.pallas import tpu as pltpu
from jax.sharding import PartitionSpec as P

HEAD_DIM = 128
MESH = pl.DeviceIdType.MESH
ANY = pl.ANY
VMEM_LIMIT = 67_043_328


class Place:
    def __init__(self, n_tp, n_sp):
        self.n_tp, self.n_sp, self.n_x = n_tp, n_sp, n_sp // 2
        self.tp, self.sp = lax.axis_index("tp"), lax.axis_index("sp")
        self.chip, self.core = self.sp // 2, self.sp % 2
        self.sib = self.chip * 2 + 1 - self.core
        self.up, self.down = (self.tp + 1) % n_tp, (self.tp + n_tp - 1) % n_tp
        self.right, self.left = self.at(1, 0), self.at(-1, 0)

    def chip_at(self, r):
        return (self.chip + r + self.n_x) % self.n_x

    def at(self, r, d):
        return self.chip_at(r) * 2 + (self.core if d == 0 else 1 - self.core)

    def barrier(self):
        sem = pltpu.get_barrier_semaphore()
        for j in range(1, self.n_sp):
            pl.semaphore_signal(sem, inc=1, device_id={"sp": (self.sp + j) % self.n_sp}, device_id_type=MESH)
        for peer in (self.up, self.down):
            pl.semaphore_signal(sem, inc=1, device_id={"tp": peer}, device_id_type=MESH)
        pl.semaphore_wait(sem, self.n_sp + 1)


def remote(src, dst, send, recv, **peer):
    return pltpu.make_async_remote_copy(
        src_ref=src, dst_ref=dst, send_sem=send, recv_sem=recv, device_id=peer, device_id_type=MESH
    )


class Ring:
    HALF = (0, 1, 0, 1, 0, 1)

    def __init__(self, axis, me, ahead, behind, far, own, slots, rows, send, recv):
        self.half = (pl.ds(0, rows // 2), pl.ds(rows // 2, rows // 2))
        self.axis, self.me, self.ahead, self.behind, self.far = axis, me, ahead, behind, far
        self.own, self.slots, self.send, self.recv = own, slots, send, recv

    def copy(self, k):
        h = self.half[self.HALF[k]]
        if k in (2, 5):
            src = dst = self.landed(k - 2)
        else:
            src, dst = self.own.at[h], self.slots(self.me).at[h]
        peer = self.ahead if k < 3 else self.behind
        return remote(src, dst, self.send.at[k], self.recv.at[k], **{self.axis: peer})

    def landed(self, k):
        origin = (self.behind, self.behind, self.far, self.ahead, self.ahead, self.far)[k]
        return self.slots(origin).at[self.half[self.HALF[k]]]

    def start(self, *ks):
        for k in ks or (0, 3, 1, 4):
            self.copy(k).start()

    def forward(self):
        for k in (0, 3):
            self.copy(k).wait_recv()
            self.copy(k + 2).start()

    def wait(self, *ks):
        for k in ks:
            self.copy(k).wait_recv()

    def drain(self):
        for k in range(6):
            self.copy(k).wait_send()


class WeightGather:
    def __init__(self, p, own, slots, rows, send, recv, sib_send, sib_recv):
        self.p, self.send, self.recv = p, sib_send, sib_recv
        self.ring = Ring("sp", p.sp, p.right, p.left, p.at(2, 0), own, slots, rows, send, recv)
        self.own = remote(own, slots(p.sp), sib_send.at[6], sib_recv.at[6], sp=p.sib)

    def to_sibling(self, k):
        block = self.ring.landed(k)
        return remote(block, block, self.send.at[k], self.recv.at[k], sp=self.p.sib)

    def forward(self):
        self.ring.forward()
        self.share(0, 3)

    def share(self, *ks):
        for k in ks:
            self.to_sibling(k).start()

    def wait_sibling(self, *ks):
        for k in ks:
            self.to_sibling(k).wait_recv()

    def drain(self):
        self.ring.drain()
        self.own.wait_send()
        for k in range(6):
            self.to_sibling(k).wait_send()


LOWEST = -0.7 * 3.4028235e38
APART = 1e38


def attend(coef, q, keys, values_t, row0, last, scores, exps, probs, tops):
    q_tile = q.shape[0]
    k_tile = scores.shape[0]
    lanes = slice(0, q_tile)

    def score(j):
        scores[:, lanes] = lax.dot_general(keys(j), q, (((1,), (1,)), ((), ())), preferred_element_type=jnp.float32)

    def body(edge, j, carry):
        top, total = carry
        s = scores[:, lanes]
        if not edge:
            score(j + 1)
        else:
            key = j * k_tile + lax.broadcasted_iota(jnp.int32, s.shape, 0)
            row = row0 + lax.broadcasted_iota(jnp.int32, s.shape, 1)
            s = jnp.where(key <= row, s, LOWEST)
        new = jnp.maximum(top, jnp.max(s, axis=0, keepdims=True))
        e = jnp.exp2((s - new) * coef)
        exps[j, :, lanes] = e
        tops[j, :, lanes] = new
        total = total * jnp.exp2((top - new) * coef) + jnp.sum(e, axis=0, keepdims=True)
        return new, total

    carry = (jnp.full((1, q_tile), LOWEST, jnp.float32), jnp.zeros((1, q_tile), jnp.float32))
    score(0)
    carry = lax.fori_loop(0, last, functools.partial(body, False), carry)
    top, total = body(True, last, carry)
    inverse = 1.0 / total

    def prob(j):
        share = jnp.exp2((tops[j, :, lanes] - top) * coef) * inverse
        return (exps[j, :, lanes] * share).astype(jnp.bfloat16)

    def weigh(j, o):
        p = probs[:, lanes]
        probs[:, lanes] = prob(j + 1)
        return o + jnp.dot(values_t[j], p, preferred_element_type=jnp.float32)

    probs[:, lanes] = prob(0)
    o = lax.fori_loop(0, last, weigh, jnp.zeros((HEAD_DIM, q_tile), jnp.float32))
    return o + jnp.dot(values_t[last], probs[:, lanes], preferred_element_type=jnp.float32)


def beside_docs(q, docs):
    return jnp.concatenate([q, ((docs.astype(jnp.float32) - 1.0) * APART).astype(q.dtype)], axis=1)


def qkv_kernel(n_tp, n_sp, coef, n_done, x_ref, w_ref, seg_ref, o_out, docs_out, m_out, seg_out, skv, sq, w_all,
               x_all, acc, qkv, w_tile, seg_all, m_all, values_t, docs, o_all, scores, exps, probs, tops,
               local_sem, tile_sem, x_send, x_recv, w_send, w_recv, w_sib_send, w_sib_recv, seg_send, seg_recv,
               main_send, main_recv, kv_send, kv_recv, q_send, q_recv, own_sem, o_sem):
    p = Place(n_tp, n_sp)
    rows, x_cols = x_ref.shape
    w_rows = w_ref.shape[0]
    n_main, _, tile = acc.shape
    n_tiles = n_main + 1
    head = 3 * HEAD_DIM
    n_shared = 2 * n_tiles - n_sp
    parts = n_sp // n_shared
    q_rows = rows // parts
    m_tile = min(rows, 256)
    n_keys, k_tile, q_tile = exps.shape
    seq = n_sp * rows
    n_docs = 4
    p.barrier()

    x_own = pltpu.make_async_copy(x_ref, x_all.at[p.tp], local_sem.at[0])
    x_own.start()
    seg_own = pltpu.make_async_copy(seg_ref, seg_all.at[p.sp], local_sem.at[1])
    seg_own.start()
    x_ring = Ring("tp", p.tp, p.up, p.down, (p.tp + 2) % n_tp, x_ref, lambda i: x_all.at[i], rows, x_send, x_recv)

    def gather(g):
        c = pl.ds(0, n_main * tile) if g == 0 else pl.ds(n_main * tile, tile)
        return WeightGather(p, w_ref.at[:, c], lambda i: w_all.at[i, :, c], w_rows, w_send.at[g], w_recv.at[g],
                            w_sib_send.at[g], w_sib_recv.at[g])

    mains, shared = gather(0), gather(1)
    mains.ring.start()
    x_ring.start()
    mains.own.start()
    shared.own.start()
    seg_copies = []
    for j in range(1, n_sp):
        copy = remote(seg_ref, seg_all.at[p.sp], seg_send.at[j - 1], seg_recv.at[j - 1], sp=(p.sp + j) % n_sp)
        copy.start()
        seg_copies.append(copy)

    def tile_load(w_src, t, slot):
        return pltpu.make_async_copy(
            w_src.at[:, pl.ds(pl.multiple_of(t * tile, tile), tile)], w_tile.at[slot], tile_sem.at[slot])

    def product(shard, m, slot):
        r = pl.ds(pl.multiple_of(m * m_tile, m_tile), m_tile)
        c = pl.ds(pl.multiple_of((shard % 2) * w_rows, w_rows), w_rows)
        return r, jnp.dot(x_all[shard // 2, r, c], w_tile[slot], preferred_element_type=jnp.float32)

    def source(shard, own=False):
        return w_ref if own else w_all.at[shard]

    def accumulate(w_src, shard, first=False):
        tile_load(w_src, 0, 0).start()

        @pl.loop(0, n_main)
        def _(t):
            slot = t % 2
            tile_load(w_src, t, slot).wait()

            @pl.when(t + 1 < n_main)
            def _():
                tile_load(w_src, t + 1, 1 - slot).start()

            @pl.loop(0, rows // m_tile)
            def _(m):
                r, d = product(shard, m, slot)
                if first:
                    acc[t, r] = d
                else:
                    acc[t, r] += d

    x_ring.forward()
    mains.forward()
    x_ring.wait(1, 4, 2, 5)
    mains.ring.wait(1, 4)
    mains.share(1, 4)
    x_own.wait()
    accumulate(w_ref, p.sp, first=True)
    mains.own.wait_recv()
    accumulate(w_all.at[p.sib], p.sib)
    accumulate(w_all.at[p.left], p.left)
    accumulate(w_all.at[p.right], p.right)
    mains.wait_sibling(0, 1)
    accumulate(w_all.at[p.at(-1, 1)], p.at(-1, 1))
    mains.wait_sibling(3, 4)
    accumulate(w_all.at[p.at(1, 1)], p.at(1, 1))
    shared.ring.start(0, 3)
    mains.ring.wait(2, 5)
    mains.share(2, 5)
    accumulate(w_all.at[p.at(2, 0)], p.at(2, 0))
    mains.wait_sibling(2, 5)

    last = p.at(2, 1)
    offsets = (2, 1, -1, 0)
    main_copies = []
    tile_load(w_all.at[last], p.chip_at(2), 0).start()
    for i, r in enumerate(offsets):
        t, slot = p.chip_at(r), i % 2
        tile_load(w_all.at[last], t, slot).wait()
        if i + 1 < n_main:
            tile_load(w_all.at[last], p.chip_at(offsets[i + 1]), 1 - slot).start()

        @pl.loop(0, rows // m_tile)
        def _(m):
            rr, d = product(last, m, slot)
            qkv[t, rr] = (acc[t, rr] + d).astype(qkv.dtype)

        for d in (0, 1):
            core = p.core if d == 0 else 1 - p.core
            src = qkv.at[t, :, pl.ds(pl.multiple_of(core * head, head), head)]
            if r == 0 and d == 0:
                copy = pltpu.make_async_copy(src, m_all.at[p.sp], own_sem.at[0])
            else:
                j = (r % 4) * 2 + d
                copy = remote(src, m_all.at[p.sp], main_send.at[j], main_recv.at[j], sp=p.at(r, d))
            copy.start()
            main_copies.append((copy, r == 0 and d == 0))

    shared.ring.start(1, 4)
    shared.forward()

    def accumulate_shared(a, b, a_own=False, step=0):
        for slot, (shard, own) in enumerate(((a, a_own), (b, False))):
            tile_load(source(shard, own), n_main, slot).start()
        for slot, (shard, own) in enumerate(((a, a_own), (b, False))):
            tile_load(source(shard, own), n_main, slot).wait()

        @pl.loop(0, rows // m_tile)
        def _(m):
            r, d = product(a, m, 0)
            d += product(b, m, 1)[1]
            if step == 0:
                acc[0, r] = d
            elif step == 1:
                acc[0, r] += d
            else:
                qkv[n_main, r] = (acc[0, r] + d).astype(qkv.dtype)

    shared.own.wait_recv()
    accumulate_shared(p.sp, p.sib, a_own=True)

    for copy in seg_copies:
        copy.wait()
    seg_own.wait()
    seg = seg_all[...]
    lane = lax.broadcasted_iota(jnp.int32, (1, HEAD_DIM), 1)
    begin = jnp.zeros((1, HEAD_DIM), jnp.float32)
    end = jnp.where(lane == n_docs - 1, jnp.float32(seq), 0.0)
    for d in range(1, n_docs):
        below = jnp.sum(jnp.where(seg < d, 1.0, 0.0), axis=0)
        below = jnp.sum(jnp.sum(below, axis=0, keepdims=True), axis=1, keepdims=True)
        begin += jnp.where(lane == d, below, 0.0)
        end += jnp.where(lane == d - 1, below, 0.0)

    @pl.loop(0, n_keys)
    def _(j):
        row = (j * k_tile + lax.broadcasted_iota(jnp.int32, (k_tile, HEAD_DIM), 0)).astype(jnp.float32)
        docs[j] = jnp.where((row >= begin) & (row < end), 1.0, 0.0).astype(docs.dtype)

    docs_copy = pltpu.make_async_copy(docs, docs_out, own_sem.at[3])
    docs_copy.start()

    seg_copy = pltpu.make_async_copy(seg_all, seg_out, own_sem.at[4])
    seg_copy.start()

    for copy, local in main_copies:
        if local:
            copy.wait()
        else:
            copy.wait_recv()
    m_copy = pltpu.make_async_copy(m_all, m_out, own_sem.at[5])
    m_copy.start()
    per = rows // k_tile

    @pl.loop(0, n_keys)
    def _(j):
        r = pl.ds(pl.multiple_of((j % per) * k_tile, k_tile), k_tile)
        values_t[j] = m_all[j // per, r, 2 * HEAD_DIM:].T

    def keys(j):
        r = pl.ds(pl.multiple_of((j % per) * k_tile, k_tile), k_tile)
        return jnp.concatenate([m_all[j // per, r, HEAD_DIM:2 * HEAD_DIM], docs[j]], axis=1)

    def o_copy(i):
        r = pl.ds(pl.multiple_of(i * q_tile, q_tile), q_tile)
        return pltpu.make_async_copy(o_all.at[r], o_out.at[r], o_sem.at[i])

    def main_attention(lo, hi):
        @pl.loop(lo, hi)
        def _(i):
            r = pl.ds(pl.multiple_of((i % per) * k_tile, k_tile), k_tile)
            q = beside_docs(m_all[i // per, r, :HEAD_DIM], docs[i])
            o = attend(coef, q, keys, values_t, i * q_tile, i, scores, exps, probs, tops)
            o_all[pl.ds(pl.multiple_of(i * q_tile, q_tile), q_tile)] = o.T.astype(o_all.dtype)
            o_copy(i).start()

    early = n_done * 5 // 7
    main_attention(0, early)

    shared.ring.wait(1, 4, 2, 5)
    shared.share(1, 4, 2, 5)
    shared.wait_sibling(0, 1)
    accumulate_shared(p.left, p.at(-1, 1), step=1)
    shared.wait_sibling(3, 4)
    accumulate_shared(p.right, p.at(1, 1), step=1)
    shared.wait_sibling(2, 5)
    accumulate_shared(p.at(2, 0), p.at(2, 1), step=2)

    shared_copies = []
    t = n_main
    for r in (2, 1, -1, 0):
        base = (p.chip_at(r) * 2 // parts) * head
        kv_src = qkv.at[t, :, pl.ds(pl.multiple_of(base + HEAD_DIM, HEAD_DIM), 2 * HEAD_DIM)]
        k = r % 4
        if r == 0:
            copy = pltpu.make_async_copy(kv_src, skv.at[p.sp], own_sem.at[1])
            copy.start()
            shared_copies.append((copy, True))
        copy = remote(kv_src, skv.at[p.sp], kv_send.at[k], kv_recv.at[k], sp=p.sib if r == 0 else p.at(r, 0))
        copy.start()
        shared_copies.append((copy, False if r == 0 else None))
        for d in (0, 1):
            dst = p.at(r, d)
            q_src = qkv.at[t, pl.ds(pl.multiple_of((dst % parts) * q_rows, q_rows), q_rows),
                           pl.ds(pl.multiple_of(base, HEAD_DIM), HEAD_DIM)]
            if r == 0 and d == 0:
                copy = pltpu.make_async_copy(q_src, sq.at[p.sp], own_sem.at[2])
            else:
                j = k * 2 + d
                copy = remote(q_src, sq.at[p.sp], q_send.at[j], q_recv.at[j], sp=dst)
            copy.start()
            shared_copies.append((copy, r == 0 and d == 0))

    main_attention(early, n_done)

    relays = []
    for r in (1, -1, 2):
        k = r % 4
        arrived = skv.at[p.at(-r, 0)]
        remote(arrived, arrived, kv_send.at[k], kv_recv.at[k], sp=p.at(r, 0)).wait_recv()
        relay = remote(arrived, arrived, kv_send.at[3 + k], kv_recv.at[3 + k], sp=p.sib)
        relay.start()
        relays.append(relay)
    for copy, local in shared_copies:
        if local:
            copy.wait()
        else:
            copy.wait_send()
            if local is False:
                copy.wait_recv()
    for relay in relays:
        relay.wait()
    for copy, local in main_copies:
        if not local:
            copy.wait_send()
    for i in range(n_done):
        o_copy(i).wait()
    docs_copy.wait()
    seg_copy.wait()
    m_copy.wait()
    x_ring.drain()
    mains.drain()
    shared.drain()


def tail_kernel(coef, n_done, tab, m_ref, o_in, o_ref, vt, scores, exps, probs, tops):
    del o_in
    step = pl.program_id(0)
    seq = m_ref.shape[0]
    _, k_tile, _ = exps.shape
    n_bounds = tab.shape[0]

    @pl.when(step == 0)
    def _():
        @pl.loop(0, seq // k_tile)
        def _(j):
            r = pl.ds(pl.multiple_of(j * k_tile, k_tile), k_tile)
            vt[j] = m_ref[r, 2 * HEAD_DIM:].T

    def doc_start(row):
        start = row * 0
        for d in range(n_bounds):
            start = jnp.where(row >= tab[d], tab[d], start)
        return start

    def attend_tail(q, k_ref, k_col, vt_ref, row0, out):
        q_tile = q.shape[0]
        lanes = slice(0, q_tile)
        row = row0 + lax.broadcasted_iota(jnp.int32, (1, q_tile), 1)
        start = doc_start(row)
        first = doc_start(row0) // k_tile
        last = row0 // k_tile
        clear = (doc_start(row0 + q_tile - 1) + k_tile - 1) // k_tile
        clear = jnp.minimum(clear, last)

        def score(j):
            r = pl.ds(pl.multiple_of(j * k_tile, k_tile), k_tile)
            scores[:, lanes] = lax.dot_general(k_ref[r, k_col:k_col + HEAD_DIM], q, (((1,), (1,)), ((), ())),
                                               preferred_element_type=jnp.float32)

        def body(edge, j, carry):
            top, total = carry
            s = scores[:, lanes]
            if edge != "last":
                score(j + 1)
            if edge:
                key = j * k_tile + lax.broadcasted_iota(jnp.int32, s.shape, 0)
                seen = key >= start
                if edge == "last":
                    seen &= key <= row
                s = jnp.where(seen, s, LOWEST)
            new = jnp.maximum(top, jnp.max(s, axis=0, keepdims=True))
            e = jnp.exp2((s - new) * coef)
            exps[j, :, lanes] = e
            tops[j, :, lanes] = new
            total = total * jnp.exp2((top - new) * coef) + jnp.sum(e, axis=0, keepdims=True)
            return new, total

        carry = (jnp.full((1, q_tile), LOWEST, jnp.float32), jnp.zeros((1, q_tile), jnp.float32))
        score(first)
        carry = lax.fori_loop(first, clear, functools.partial(body, "first"), carry)
        carry = lax.fori_loop(clear, last, functools.partial(body, ""), carry)
        top, total = body("last", last, carry)
        inverse = 1.0 / total

        def prob(j):
            share = jnp.exp2((tops[j, :, lanes] - top) * coef) * inverse
            return (exps[j, :, lanes] * share).astype(jnp.bfloat16)

        def weigh(j, o):
            p = probs[:, lanes]
            probs[:, lanes] = prob(j + 1)
            return o + jnp.dot(vt_ref[j], p, preferred_element_type=jnp.float32)

        probs[:, lanes] = prob(first)
        o = lax.fori_loop(first, last, weigh, jnp.zeros((HEAD_DIM, q_tile), jnp.float32))
        o = o + jnp.dot(vt_ref[last], probs[:, lanes], preferred_element_type=jnp.float32)
        out[...] = o.T.astype(out.dtype)

    q_tile = o_ref.shape[0]
    row0 = (step + n_done) * q_tile
    q = m_ref[pl.ds(pl.multiple_of(row0, q_tile), q_tile), :HEAD_DIM]
    attend_tail(q, m_ref, HEAD_DIM, vt, row0, o_ref)


def out_kernel(n_tp, n_sp, coef, o_ref, docs_ref, skv_ref, sq_ref, w_ref, y_ref, ctx, w_all, acc, skv, sq, docs,
               values_t, so_all, scores, exps, probs, tops, local_sem, w_send, w_recv, w_sib_send, w_sib_recv,
               o_send, o_recv, s_send, s_recv, c_send, c_recv):
    p = Place(n_tp, n_sp)
    n_x = p.n_x
    _, rows, local = ctx.shape
    w_rows = w_ref.shape[0]
    n_shared = local // HEAD_DIM - n_sp
    parts = n_sp // n_shared
    q_rows = rows // parts
    m_tile = min(rows, 256)
    pair = 2 * HEAD_DIM
    n_keys, k_tile, _ = exps.shape
    per = rows // k_tile

    loads = [pltpu.make_async_copy(src, dst, local_sem.at[3 + i])
             for i, (src, dst) in enumerate(((skv_ref, skv), (sq_ref, sq), (docs_ref, docs)))]
    for load in loads:
        load.start()
    w_own = pltpu.make_async_copy(w_ref, w_all.at[p.sp], local_sem.at[0])
    w_own.start()
    p.barrier()

    def head_copy(r, d):
        dst = p.at(r, d)
        src = o_ref.at[pl.ds(pl.multiple_of(dst * rows, rows), rows)]
        to = ctx.at[p.tp, :, pl.ds(pl.multiple_of(p.sp * HEAD_DIM, HEAD_DIM), HEAD_DIM)]
        if r == 0 and d == 0:
            return pltpu.make_async_copy(src, to, local_sem.at[1])
        j = (r % 4) * 2 + d
        return remote(src, to, o_send.at[j], o_recv.at[j], sp=dst)

    def shared_copy(r, d):
        dst = p.at(r, d)
        src = so_all.at[pl.ds(pl.multiple_of(dst * q_rows, q_rows), q_rows)]
        to = ctx.at[p.tp, pl.ds(pl.multiple_of((p.sp % parts) * q_rows, q_rows), q_rows),
                    pl.ds(pl.multiple_of((n_sp + p.sp // parts) * HEAD_DIM, HEAD_DIM), HEAD_DIM)]
        if r == 0 and d == 0:
            return pltpu.make_async_copy(src, to, local_sem.at[2])
        j = (r % 4) * 2 + d
        return remote(src, to, s_send.at[j], s_recv.at[j], sp=dst)

    peers = [(r, d) for r in (0, 1, -1, 2) for d in (0, 1)]
    for r, d in peers:
        head_copy(r, d).start()
    weight = WeightGather(p, w_ref, lambda i: w_all.at[i], w_rows, w_send, w_recv, w_sib_send, w_sib_recv)
    weight.ring.start(0, 3)
    weight.own.start()

    def ring(i, column):
        c = pl.ds(pl.multiple_of(column, pair), pair)
        return Ring("tp", p.tp, p.up, p.down, (p.tp + 2) % n_tp, ctx.at[p.tp, :, c], lambda j: ctx.at[j, :, c], rows,
                    c_send.at[i], c_recv.at[i])

    def wait_in(copy, local):
        if local:
            copy.wait()
        else:
            copy.wait_recv()

    rings = []

    def start_ring(i, r):
        for d in (0, 1):
            wait_in(head_copy(r, d), r == 0 and d == 0)
        rings.append(ring(i, p.chip_at(-r) * pair))
        rings[-1].start()

    def keys(j):
        r = pl.ds(pl.multiple_of((j % per) * k_tile, k_tile), k_tile)
        return jnp.concatenate([skv[j // per, r, :HEAD_DIM], docs[j]], axis=1)

    def shared_attention(lo, hi):
        @pl.loop(lo, hi)
        def _(i):
            row0 = (i * parts + p.sp % parts) * q_rows
            j = row0 // k_tile
            r = pl.ds(pl.multiple_of(row0 % k_tile, q_rows), q_rows)
            q = beside_docs(sq[i], docs[j, r])
            o = attend(coef, q, keys, values_t, row0, j, scores, exps, probs, tops)
            so_all[pl.ds(pl.multiple_of(i * q_rows, q_rows), q_rows)] = o.T.astype(so_all.dtype)

    start_ring(0, 0)
    for load in loads:
        load.wait()

    @pl.loop(0, n_keys)
    def _(j):
        r = pl.ds(pl.multiple_of((j % per) * k_tile, k_tile), k_tile)
        values_t[j] = skv[j // per, r, HEAD_DIM:].T

    shared_attention(0, n_sp // 2)
    start_ring(1, 1)
    start_ring(2, -1)
    shared_attention(n_sp // 2, n_sp)
    for r, d in peers:
        shared_copy(r, d).start()
    weight.ring.start(1, 4)
    start_ring(3, 2)
    rings[0].forward()
    rings[1].forward()
    rings[2].forward()
    weight.forward()
    for r, d in peers:
        wait_in(shared_copy(r, d), r == 0 and d == 0)
    rings.append(ring(n_x, n_sp * HEAD_DIM))
    rings[-1].start()
    for c in rings[3:]:
        c.forward()
    weight.ring.wait(1, 4)
    weight.share(1, 4)
    for c in rings:
        c.wait(1, 4)
    w_own.wait()
    weight.own.wait_recv()
    weight.wait_sibling(0, 1, 3, 4)

    def block(j, step):
        @pl.loop(0, rows // m_tile)
        def _(m):
            r = pl.ds(pl.multiple_of(m * m_tile, m_tile), m_tile)
            d = jnp.dot(ctx[j, r, :w_rows], w_all[2 * j], preferred_element_type=jnp.float32)
            d += jnp.dot(ctx[j, r, w_rows:], w_all[2 * j + 1], preferred_element_type=jnp.float32)
            if step == 0:
                acc[r] = d
            elif step < n_tp - 1:
                acc[r] += d
            else:
                y_ref[r] = (acc[r] + d).astype(y_ref.dtype)

    turn = (p.chip + n_x - p.tp) % n_x
    far = turn // 2
    block((p.tp + far * (1 - turn % 2)) % n_tp, 0)
    block((p.tp + 1 + 2 * far) % n_tp, 1)
    weight.ring.wait(2, 5)
    weight.share(2, 5)
    weight.wait_sibling(2, 5)
    block((p.tp + far * (turn - 2) + (1 - far) * 3) % n_tp, 2)
    for c in rings:
        c.wait(2, 5)
    block((p.tp + 2) % n_tp, 3)

    for c in rings:
        c.drain()
    weight.drain()
    for r, d in peers:
        if not (r == 0 and d == 0):
            head_copy(r, d).wait_send()
            shared_copy(r, d).wait_send()


def solution(mesh):
    n_tp, n_sp = mesh.shape["tp"], mesh.shape["sp"]
    dma = pltpu.SemaphoreType.DMA
    hbm = pl.BlockSpec(memory_space=ANY)
    coef = 1.0 / HEAD_DIM ** 0.5 * 1.4426950408889634

    def params(collective_id):
        return pltpu.CompilerParams(collective_id=collective_id, has_side_effects=True, vmem_limit_bytes=VMEM_LIMIT)

    def local_block(x_blk, wqkv_blk, wout_blk, seg_blk):
        rows, x_cols = x_blk.shape
        w_rows, n_cols = wqkv_blk.shape
        head = 3 * HEAD_DIM
        heads = n_cols // head
        local = heads * HEAD_DIM
        parts = n_sp // (heads - n_sp)
        q_rows = rows // parts
        tile = 2 * head
        n_tiles = n_cols // tile
        n_main = n_tiles - 1
        seq = n_sp * rows
        q_tile = k_tile = 2 * q_rows
        n_keys = seq // k_tile
        bf16, f32 = x_blk.dtype, jnp.float32
        seg = seg_blk.reshape(rows // 128, 128)

        def attention_scratch(q):
            return [
                pltpu.VMEM((k_tile, q), f32),
                pltpu.VMEM((n_keys, k_tile, q), f32),
                pltpu.VMEM((k_tile, q), bf16),
                pltpu.VMEM((n_keys, 1, q), f32),
            ]

        n_done = n_keys * 7 // 16
        o_main, docs, m_all, seg_all, skv, sq, _ = pl.pallas_call(
            functools.partial(qkv_kernel, n_tp, n_sp, coef, n_done),
            out_shape=(
                jax.ShapeDtypeStruct((seq, HEAD_DIM), bf16),
                jax.ShapeDtypeStruct((n_keys, k_tile, HEAD_DIM), bf16),
                jax.ShapeDtypeStruct((n_sp, rows, head), bf16),
                jax.ShapeDtypeStruct((n_sp,) + seg.shape, seg.dtype),
                jax.ShapeDtypeStruct((n_sp, rows, 2 * HEAD_DIM), bf16),
                jax.ShapeDtypeStruct((n_sp, q_rows, HEAD_DIM), bf16),
                jax.ShapeDtypeStruct((n_sp, w_rows, n_cols), bf16),
            ),
            in_specs=[hbm] * 3,
            out_specs=(hbm,) * 7,
            scratch_shapes=[
                pltpu.VMEM((n_tp, rows, x_cols), bf16),
                pltpu.VMEM((n_main, rows, tile), f32),
                pltpu.VMEM((n_tiles, rows, tile), bf16),
                pltpu.VMEM((2, w_rows, tile), bf16),
                pltpu.VMEM((n_sp,) + seg.shape, seg.dtype),
                pltpu.VMEM((n_sp, rows, head), bf16),
                pltpu.VMEM((n_keys, HEAD_DIM, k_tile), bf16),
                pltpu.VMEM((n_keys, k_tile, HEAD_DIM), bf16),
                pltpu.VMEM((seq, HEAD_DIM), bf16),
                *attention_scratch(q_tile),
                dma((2,)), dma((2,)), dma((6,)), dma((6,)), dma((2, 6)), dma((2, 6)), dma((2, 7)), dma((2, 7)),
                dma((n_sp - 1,)), dma((n_sp - 1,)), dma((8,)), dma((8,)), dma((7,)), dma((7,)), dma((8,)), dma((8,)),
                dma((6,)), dma((n_keys,)),
            ],
            compiler_params=params(0),
            name="qkv",
        )(x_blk, wqkv_blk, seg)

        seg_ids = jnp.arange(1, 4, dtype=seg_all.dtype)[:, None]
        starts = jnp.sum((seg_all.reshape(1, seq) < seg_ids).astype(jnp.int32), axis=1)
        o_main = pl.pallas_call(
            functools.partial(tail_kernel, coef, n_done),
            out_shape=jax.ShapeDtypeStruct((seq, HEAD_DIM), bf16),
            grid_spec=pltpu.PrefetchScalarGridSpec(
                num_scalar_prefetch=1,
                grid=(n_keys - n_done,),
                in_specs=[pl.BlockSpec((seq, head), lambda i, t: (0, 0), pipeline_mode=pl.Buffered(1)), hbm],
                out_specs=pl.BlockSpec((q_tile, HEAD_DIM), lambda i, t: (i + n_done, 0)),
                scratch_shapes=[pltpu.VMEM((n_keys, HEAD_DIM, k_tile), bf16), *attention_scratch(q_tile)],
            ),
            input_output_aliases={2: 0},
            compiler_params=pltpu.CompilerParams(dimension_semantics=("arbitrary",), vmem_limit_bytes=VMEM_LIMIT),
            name="tail",
        )(starts, m_all.reshape(seq, head), o_main)

        wo_rows, wo_cols = wout_blk.shape
        n_rings = local // (2 * HEAD_DIM)
        return pl.pallas_call(
            functools.partial(out_kernel, n_tp, n_sp, coef),
            out_shape=jax.ShapeDtypeStruct((rows, wo_cols), bf16),
            in_specs=[hbm] * 5,
            out_specs=pl.BlockSpec(memory_space=pltpu.VMEM),
            scratch_shapes=[
                pltpu.VMEM((n_tp, rows, local), bf16),
                pltpu.VMEM((n_sp, wo_rows, wo_cols), bf16),
                pltpu.VMEM((rows, wo_cols), f32),
                pltpu.VMEM((n_sp, rows, 2 * HEAD_DIM), bf16),
                pltpu.VMEM((n_sp, q_rows, HEAD_DIM), bf16),
                pltpu.VMEM((n_keys, k_tile, HEAD_DIM), bf16),
                pltpu.VMEM((n_keys, HEAD_DIM, k_tile), bf16),
                pltpu.VMEM((seq // parts, HEAD_DIM), bf16),
                *attention_scratch(q_rows),
                dma((6,)), dma((6,)), dma((6,)), dma((7,)), dma((7,)),
                dma((8,)), dma((8,)), dma((8,)), dma((8,)), dma((n_rings, 6)), dma((n_rings, 6)),
            ],
            compiler_params=params(1),
            name="out",
        )(o_main, docs, skv, sq, wout_blk)

    row_spec = P(("dp", "sp"), "tp")
    return jax.shard_map(
        local_block, mesh=mesh, in_specs=(row_spec, P("sp", "tp"), P("sp", "tp"), P(("dp", "sp"))),
        out_specs=row_spec, check_vma=False)
```
